128 devices in a mesh: rep: 1, dp: 128 (over x, y, z, core).
Axes of the slice: x: 4, y: 4, z: 4, core: 2. Of those that a mesh axis runs over, the one named last changes fastest.
Arguments:
- x: bfloat16 [128, 1024, 1280], P(('rep', 'dp'))
- dy: bfloat16 [128, 1024, 1280], P(('rep', 'dp'))
- w_gate: bfloat16 [2, 1280, 3072], replicated
- w_up: bfloat16 [2, 1280, 3072], replicated
- w_down: bfloat16 [2, 3072, 1280], replicated
- m_w_gate: float32 [2, 1280, 3072], P(None, 'dp')
- m_w_up: float32 [2, 1280, 3072], P(None, 'dp')
- m_w_down: float32 [2, 3072, 1280], P(None, 'dp')
- v_w_gate: float32 [2, 1280, 3072], P(None, 'dp')
- v_w_up: float32 [2, 1280, 3072], P(None, 'dp')
- v_w_down: float32 [2, 3072, 1280], P(None, 'dp')
Outputs:
- output 1: bfloat16 [2, 1280, 3072], P('rep')
- output 2: bfloat16 [2, 1280, 3072], P('rep')
- output 3: bfloat16 [2, 3072, 1280], P('rep')
- output 4: float32 [2, 1280, 3072], P('rep', 'dp')
- output 5: float32 [2, 1280, 3072], P('rep', 'dp')
- output 6: float32 [2, 3072, 1280], P('rep', 'dp')
- output 7: float32 [2, 1280, 3072], P('rep', 'dp')
- output 8: float32 [2, 1280, 3072], P('rep', 'dp')
- output 9: float32 [2, 3072, 1280], P('rep', 'dp')
All inputs are finite; a program needn't handle non-finite values.
Results may differ from the reference program's by a relative error of at most 0.022.
Values are sent between devices in bfloat16 or wider.
A program may use at most 1.5 GiB of HBM per device.

```python
import jax
import jax.numpy as jnp
from jax import lax

SEQUENCES = 128
TOKENS = 1024
D = 1280
FF = 3072
LAYERS = 2
NAMES = ("w_gate", "w_up", "w_down")
SHAPES = {"w_gate": (LAYERS, D, FF), "w_up": (LAYERS, D, FF), "w_down": (LAYERS, FF, D)}


def bump(key, n, height):
    away = (jnp.arange(n, dtype=jnp.int32) - jax.random.randint(key, (), 0, n, jnp.int32)) % n
    return jnp.where(away < n // 8, height, 1.0)


def together(key, own, strength):
    shared = jax.random.normal(key, own.shape[1:], jnp.float32)
    return (own + strength * shared) * lax.rsqrt(1 + strength * strength)


def setup_inputs(seed: int = 0, part: int = 0) -> dict:
    kx, kdy, ka, kb, kz, kf, kh, kl, *keys = jax.random.split(jax.random.key(seed), 8 + 3 * len(NAMES))
    kx, kdy, ka, kb = (jax.random.fold_in(k, part) for k in (kx, kdy, ka, kb))
    kw, km, kv = (keys[i::3] for i in range(3))
    shape = (SEQUENCES, TOKENS, D)
    much_x, much_dy = jax.random.uniform(kz, (2,), jnp.float32, 0.0, 1.0)
    loud = 2.0 ** jax.random.uniform(jax.random.fold_in(kz, 1), (), jnp.float32, -1.0, 2.0)
    layers = 2.0 ** jax.random.uniform(kl, (LAYERS, 1, 1), jnp.float32, -1.0, 1.0)
    x = together(ka, jax.random.normal(kx, shape, jnp.float32), much_x) * bump(kf, D, 4.0)
    dy = together(kb, jax.random.normal(kdy, shape, jnp.float32), much_dy)
    drawn = {"x": x.astype(jnp.bfloat16), "dy": (loud * dy * (SEQUENCES * TOKENS) ** -0.5).astype(jnp.bfloat16)}
    for key, name in zip(kw, NAMES, strict=True):
        w = jax.random.normal(key, SHAPES[name], jnp.float32) * SHAPES[name][1] ** -0.5
        drawn[name] = (w * {"w_gate": 1.0, "w_up": bump(kh, FF, 4.0), "w_down": layers}[name]).astype(jnp.bfloat16)
    for key, name in zip(km, NAMES, strict=True):
        drawn[f"m_{name}"] = 0.1 * jax.random.normal(key, SHAPES[name], jnp.float32)
    for key, name in zip(kv, NAMES, strict=True):
        drawn[f"v_{name}"] = jax.random.uniform(key, SHAPES[name], jnp.float32, 0.005, 0.015)
    return drawn


def matmul(a, w):
    return jnp.dot(a, w, preferred_element_type=jnp.float32).astype(jnp.bfloat16)


def normed(h):
    wide = h.astype(jnp.float32)
    scale = lax.rsqrt(jnp.mean(wide**2, -1, keepdims=True) + 1e-6)
    return (wide * scale).astype(jnp.bfloat16)


def layer(h, w):
    a = normed(h)
    gate = jnp.dot(a, w["w_gate"], preferred_element_type=jnp.float32)
    up = jnp.dot(a, w["w_up"], preferred_element_type=jnp.float32)
    return h + matmul((jax.nn.silu(gate) * up).astype(jnp.bfloat16), w["w_down"])


def adamw(w, m, v, g):
    m = 0.9 * m + 0.1 * g
    v = 0.95 * v + 0.05 * g * g
    step = m * lax.rsqrt(v + 1e-8) + 0.1 * w
    return (w - 0.02 * step).astype(jnp.bfloat16), m, v


def clipped(gradients, sum_of_squares, count):
    factor = jnp.minimum(1.0, 0.5 * lax.rsqrt(sum_of_squares / count + 1e-30))
    return [g * factor for g in gradients]


def stack(weights, h):
    return lax.scan(lambda h, w: (layer(h, w), None), h, weights)[0]


def reference(x, dy, w_gate, w_up, w_down, m_w_gate, m_w_up, m_w_down, v_w_gate, v_w_up, v_w_down):
    weights = dict(zip(NAMES, (w_gate, w_up, w_down), strict=True))

    def take(so_far, sequence):
        h, by_y = sequence
        _, back = jax.vjp(lambda w: stack(w, h), weights)
        return jax.tree.map(lambda total, term: total + term.astype(jnp.float32), so_far, back(by_y)[0]), None

    none_yet = {name: jnp.zeros(w.shape, jnp.float32) for name, w in weights.items()}
    by_weights, _ = lax.scan(take, none_yet, (x, dy))
    gradients = [by_weights[name].astype(jnp.bfloat16).astype(jnp.float32) for name in NAMES]
    gradients = clipped(gradients, sum(jnp.sum(g * g) for g in gradients), sum(g.size for g in gradients))
    new = [
        adamw(w.astype(jnp.float32), m, v, g)
        for w, m, v, g in zip((w_gate, w_up, w_down), (m_w_gate, m_w_up, m_w_down), (v_w_gate, v_w_up, v_w_down), gradients, strict=True)
    ]
    return tuple(one[which] for which in range(3) for one in new)
```

```python
import functools

import jax
import jax.numpy as jnp
from jax import lax
from jax.experimental import pallas as pl
from jax.experimental.pallas import tpu as pltpu
from jax.sharding import PartitionSpec as P

BF, F32 = jnp.bfloat16, jnp.float32
T, D, FF = 1024, 1280, 3072
L, RING, PAIR = 2, 4, 2
X, Y, Z, CORE = range(4)
HG, HD = FF // PAIR, D // PAIR
ROWS, DROWS = D // (RING**3 * PAIR), FF // (RING**3 * PAIR)
ZROWS = PAIR * RING * ROWS
PAD = 24
MOST = 67043328
HBM, VM = pl.BlockSpec(memory_space=pltpu.HBM), pl.BlockSpec(memory_space=pltpu.VMEM)
dma, vmem = pltpu.SemaphoreType.DMA, pltpu.VMEM
out = jax.ShapeDtypeStruct


class Place:
    def __init__(self):
        i = lax.axis_index("dp")
        chip, core = lax.div(i, PAIR), lax.rem(i, PAIR)
        self.at = [[lax.div(chip, RING**2)], [lax.rem(lax.div(chip, RING), RING)], [lax.rem(chip, RING)], [core, 1 - core]]
        for steps in self.at[:CORE]:
            steps += [lax.rem(steps[0] + r, RING) for r in range(1, RING)]
        self.peers = {}

    def moved(self, dim, by=1):
        by %= len(self.at[dim])
        if (dim, by) not in self.peers:
            x, y, z, core = (steps[by if d == dim else 0] for d, steps in enumerate(self.at))
            self.peers[dim, by] = {"dp": ((x * RING + y) * RING + z) * PAIR + core}
        return self.peers[dim, by]


def meet(peers):
    barrier = pltpu.get_barrier_semaphore()
    for peer in peers:
        pl.semaphore_signal(barrier, inc=1, device_id=peer)
    pl.semaphore_wait(barrier, len(peers))


def remote(src, dst, send, recv, peer):
    return pltpu.make_async_remote_copy(src, dst, send, recv, device_id=peer)


def up(v):
    return v.astype(F32)


def call(kernel, outs, ins, scratch, name, vmem_limit=MOST, ident=None, out_specs=None, **more):
    return pl.pallas_call(
        kernel,
        out_shape=outs,
        in_specs=ins,
        out_specs=out_specs or [HBM] * len(outs),
        scratch_shapes=scratch,
        compiler_params=pltpu.CompilerParams(collective_id=ident, has_side_effects=ident is not None, vmem_limit_bytes=vmem_limit),
        name=name,
        **more,
    )


class Cut:
    def __init__(self, gate):
        self.gate = gate
        self.units = L * (PAIR if gate else 1)
        self.width = HG // 2 if gate else HD
        self.n, self.rows = (1, ZROWS) if gate else (RING, DROWS)

    def dims(self, s):
        return (s, 1 - s, Z) if self.gate else (Z, s, 1 - s)

    def part(self, s, h, base=0):
        first = 384 if self.gate or s == 0 else 256
        return pl.ds(base + first, self.width - first) if h else pl.ds(base, first)

    def index(self, here, s, dim, r, done, cols):
        at = [here.at[d][r % RING] if d == dim else slice(None) if d in done else here.at[d][0] for d in (X, Y, Z)]
        return (at[X], at[Y]) + ((slice(None),) if self.gate else (at[Z], s)) + (slice(None), cols)


GATE, DOWN = Cut(True), Cut(False)
CUTS = (GATE, DOWN)


def ahead(k):
    return 1 if k in (0, 3, 4) else -1


TILES, HALF = 6, 3
TILE = FF // TILES
TN = (((0,), (0,)), ((), ()))


def dw_kernel(a, dg, du, hid, dy, og, ou, od, va, vb, vh, vy, sd, rd, wd, sg, rg, insem, outsem, dsend, drecv, gsend, grecv):
    here = Place()
    c, other = here.at[CORE][0], here.moved(CORE)
    tile = lambda i, base=0: pl.ds(pl.multiple_of(base + i * TILE, TILE), TILE)
    loads = [pltpu.make_async_copy(dy, vy, insem.at[TILES]), pltpu.make_async_copy(a, va, insem.at[TILES + 1])]
    loads += [pltpu.make_async_copy(hid.at[:, tile(i)], vh.at[:, tile(i)], insem.at[i]) for i in range(TILES)]
    loads += [pltpu.make_async_copy(w, vb.at[i], insem.at[TILES + 2 + i]) for i, w in enumerate((dg, du))]
    for cp in loads:
        cp.start()
    meet([other])

    def dsent(i):
        return remote(sd.at[i], rd.at[i], dsend.at[i], drecv.at[i], other)

    def dout(i):
        return pltpu.make_async_copy(rd.at[i], od.at[tile(i), :], outsem.at[i])

    def dadd(i):
        dsent(i).wait_recv()
        rd[i] = (up(rd[i]) + up(wd[i])).astype(BF)
        dout(i).start()

    for cp in loads[: TILES + 2]:
        cp.wait()

    def dtile(i, _):
        full = lax.dot_general(vh[:, tile(i)], vy[...], TN, preferred_element_type=F32).astype(BF)
        low, high = full[:, :HD], full[:, HD:]
        sd[i] = jnp.where(c == 0, high, low)
        wd[i] = jnp.where(c == 0, low, high)
        dsent(i).start()
        pl.when(i > 0)(lambda: dadd(i - 1))
        return _

    lax.fori_loop(0, TILES, dtile, 0)

    def gsent(w, i):
        return remote(sg.at[w, i], rg.at[w, i], gsend.at[w, i], grecv.at[w, i], other)

    def gout(w, i):
        return pltpu.make_async_copy(rg.at[w, i], (og, ou)[w].at[:, tile(i)], outsem.at[TILES + HALF * w + i])

    for w in range(2):
        loads[TILES + 2 + w].wait()

        def product(i, half):
            cols = tile(i, half * HG)
            return lax.dot_general(va[...], vb[w, :, cols], TN, preferred_element_type=F32).astype(BF)

        def theirs(i, _):
            sg[w, i] = product(i, 1 - c)
            gsent(w, i).start()
            return _

        def mine(i, _):
            own = product(i, c)
            gsent(w, i).wait_recv()
            rg[w, i] = (up(rg[w, i]) + up(own)).astype(BF)
            gout(w, i).start()
            return _

        lax.fori_loop(0, HALF, theirs, 0)
        if w == 0:
            dadd(TILES - 1)
        lax.fori_loop(0, HALF, mine, 0)
    for i in range(TILES):
        dsent(i).wait_send()
        dout(i).wait()
        gsent(i // HALF, i % HALF).wait_send()
        gout(i // HALF, i % HALF).wait()


def dw(a, dg, du, hid, dy):
    tiles = (PAIR, HALF, D, TILE)
    return call(
        dw_kernel, [out((D, HG), BF)] * 2 + [out((FF, HD), BF)], [HBM] * 5,
        [vmem((T, D), BF), vmem((2, T, FF), BF), vmem((T, FF), BF), vmem((T, D), BF)] + [vmem((TILES, TILE, HD), BF)] * 3 + [vmem(tiles, BF)] * 2
        + [dma((TILES + 4,)), dma((2 * TILES,))] + [dma((TILES,))] * 2 + [dma((2, HALF))] * 2,
        "dw", ident=1, cost_estimate=pl.CostEstimate(flops=6 * T * D * FF, bytes_accessed=8 * T * FF, transcendentals=0),
    )(a, dg, du, hid, dy)


PHASES = 3
COPIES = 6


ALL = slice(None)


class Summed:
    def __init__(self, here, cut, src, b, u, s):
        self.here = here
        self.cut, self.src, self.us, self.s, self.dims = cut, src, (u, s), s, cut.dims(s)
        self.got, self.kept = [b[k] for k in ("r1", "r2", "r3")], [b[k] for k in ("o1", "k2", "k3")]
        self.t3, self.sems = b["t3"], (b["send"], b["recv"], b["own"])

    def block(self, phase, r, cols=ALL, first=()):
        dim = self.dims[phase]
        i = self.here.at[dim][r % RING]
        if phase == 2:
            return self.us + first + (i, ALL, cols)
        second = phase == 1 and not self.cut.gate and self.s
        return self.us + first + ((ALL, i) if second else (i, ALL)) + (ALL, cols)

    def first(self, r, h):
        cols = self.cut.part(self.s, h, self.s * self.cut.width if self.cut.gate else 0)
        u = self.us[0]
        return self.src[u if isinstance(u, int) else 0].at[self.cut.index(self.here, self.s, self.dims[0], r, self.dims, cols)]

    def at(self, phase, kind, cols=ALL):
        return self.us + (kind,) + (ALL,) * (PHASES - phase) + (cols,)

    def copy(self, phase, k):
        kind, h = k // 2, k % 2
        cols = self.cut.part(self.s, h)
        got = self.got[phase]
        r = (2, 1 if h else -1, 0)[kind]
        if kind == 2:
            src = got.at[self.at(phase, 0, cols)]
        elif phase == 0:
            src = self.first(r, h)
        elif phase == 1:
            src = self.got[0].at[self.block(1, r, cols, (2,))]
        else:
            src = self.t3.at[self.block(2, r, cols)]
        i = self.us + (phase * COPIES + k,)
        return remote(src, got.at[self.at(phase, kind, cols)], self.sems[0].at[i], self.sems[1].at[i], self.here.moved(self.dims[phase], ahead(k)))

    def own(self, k):
        kind, h = k // 2, k % 2
        src = self.first(0 if kind else ahead(h), h)
        return pltpu.make_async_copy(src, self.kept[0].at[self.at(0, kind, self.cut.part(self.s, h))], self.sems[2].at[self.us + (k,)])

    def start(self):
        for k in range(4):
            self.copy(0, k).start()
        for k in range(4):
            self.own(k).start()

    def pass_on(self, phase):
        got, kept = self.got[phase], self.kept[phase]
        for h in range(2):
            self.copy(phase, h).wait_recv()
            cols = self.cut.part(self.s, h)
            if phase:
                i = self.at(phase, 0, cols)
                got[i] = (up(got[i]) + kept[self.block(phase, ahead(h), cols)]).astype(BF)
            else:
                self.own(h).wait()

                def add(n, _):
                    i = self.us + (0, n, ALL, ALL, cols)
                    got[i] = (up(got[i]) + up(kept[i])).astype(BF)
                    return _

                lax.fori_loop(0, RING, add, 0)
            self.copy(phase, 4 + h).start()

    def finish(self, phase):
        for k in range(2, COPIES):
            self.copy(phase, k).wait_recv()
        got, kept = self.got[phase], self.kept[phase]
        if phase == 0:
            for k in (2, 3):
                self.own(k).wait()

            def add(n, _):
                total = up(kept[self.us + (1, n)]) + up(got[self.us + (2, n)]) + up(got[self.us + (1, n)])
                self.kept[1][self.us + (n,)] = total
                got[self.us + (2, n)] = total.astype(BF)
                return _

            lax.fori_loop(0, RING, add, 0)
        else:
            return kept[self.block(phase, 0)] + up(got[self.us + (2,)]) + up(got[self.us + (1,)])

    def starts(self, phase):
        for k in range(4):
            self.copy(phase, k).start()


def rs_kernel(*refs):
    nu = GATE.units + L
    ins, (og, od, onorm), refs = refs[:nu], refs[nu : nu + 3], list(refs[nu + 3 :])
    names = ("r1", "o1", "k2", "r2", "t3", "k3", "r3", "send", "recv", "own")
    bufs = []
    for _ in CUTS:
        bufs.append(dict(zip(names, refs)))
        del refs[: len(names)]
    f3, f4, ce, cr, co, fd, dr, nb, nr, csend, crecv, nsend, nrecv, putsem = refs
    here = Place()
    c, other = here.at[CORE][0], here.moved(CORE)
    meet([here.moved(d, r) for d in (X, Y, Z) for r in range(1, RING)] + [other])
    srcs = ins[: GATE.units], ins[GATE.units :]

    def streams(g, u):
        return [Summed(here, CUTS[g], srcs[g], bufs[g], u, s) for s in range(2)]

    for u in range(GATE.units):
        for st in streams(0, u) + (streams(1, u) if u < L else []):
            st.start()

    def gate_rows(st):
        f3[0:ZROWS] = st.finish(1)[0]
        for i in range(RING):
            rows = f3[i * PAIR * ROWS : i * PAIR * ROWS + PAD]
            st.kept[2][st.us + (i,)] = rows
            st.t3[st.us + (i,)] = rows.astype(BF)

    def down_rows(st):
        total = st.finish(1)
        st.kept[2][st.us] = total
        st.t3[st.us] = total.astype(BF)

    def swap_g(u):
        return remote(ce.at[u], cr.at[u], csend.at[u], crecv.at[u], other)

    def swap_d(u):
        return remote(fd.at[u, 1 - c], dr.at[u], csend.at[GATE.units + u], crecv.at[GATE.units + u], other)

    def last_g(u):
        for st in streams(0, u):
            f4[0:PAD, pl.ds(st.s * GATE.width, GATE.width)] = st.finish(2)
        low, high = f4[0:16], f4[ROWS : ROWS + 16]
        co[u] = jnp.where(c == 0, low, high).astype(BF)
        ce[u] = jnp.where(c == 0, high, low).astype(BF)
        swap_g(u).start()

    def last_d(u):
        for st in streams(1, u):
            fd[u, st.s] = st.finish(2).astype(BF)
        swap_d(u).start()

    def each(step):
        def both(u, _):
            for g in (1, 0):
                for v in range(CUTS[g].units // L):
                    step(g, u * CUTS[g].units // L + v)
            return _

        lax.fori_loop(0, L, both, 0)

    def all_streams(step):
        each(lambda g, u: [step(g, st) for st in streams(g, u)])

    f3[ZROWS : ZROWS + 8] = jnp.zeros((8, GATE.width), F32)
    f4[PAD : PAD + 8] = jnp.zeros((8, HG), F32)
    all_streams(lambda g, st: st.pass_on(0))
    all_streams(lambda g, st: (st.finish(0), st.starts(1)))
    all_streams(lambda g, st: st.pass_on(1))
    all_streams(lambda g, st: ((gate_rows, down_rows)[g](st), st.starts(2)))
    all_streams(lambda g, st: st.pass_on(2))
    each(lambda g, u: (last_g, last_d)[g](u))

    valid = lax.broadcasted_iota(jnp.int32, (16, HG), 0) < ROWS
    puts = []

    def put(src, dst):
        puts.append(pltpu.make_async_copy(src, dst, putsem.at[len(puts)]))
        puts[-1].start()

    def squares(v):
        v = v * v
        rows = functools.reduce(jnp.add, [v[i : i + 8] for i in range(0, v.shape[0], 8)])
        return functools.reduce(jnp.add, [rows[:, i : i + 128] for i in range(0, v.shape[1], 128)])

    def half(which, n):
        return pl.ds(pl.multiple_of(which * n, 128), n)

    total = jnp.zeros((8, 128), F32)
    for u in range(GATE.units):
        swap_g(u).wait_recv()
        for src, which in ((co, c), (cr, 1 - c)):
            put(src.at[u], og.at[u, :, half(which, HG)])
            total = total + squares(jnp.where(valid, up(src[u]), 0.0))
    for u in range(L):
        swap_d(u).wait_recv()
        for src, i, which in ((fd, (u, c), c), (dr, u, 1 - c)):
            put(src.at[i], od.at[u, :, half(which, HD)])
            total = total + squares(up(src[i]))
    n = 0
    for stage, dim in enumerate((CORE, Z, Y, X)):
        nb[stage] = total
        copies = []
        for r in range(1, PAIR if dim == CORE else RING):
            copies.append(remote(nb.at[stage], nr.at[n], nsend.at[n], nrecv.at[n], here.moved(dim, r)))
            copies[-1].start()
            n += 1
        for i, cp in enumerate(copies):
            cp.wait()
            total = total + nr[n - len(copies) + i]
    nb[4] = total
    put(nb.at[4], onorm)
    for g, cut in enumerate(CUTS):
        for u in range(cut.units):
            for st in streams(g, u):
                for k in range(PHASES * COPIES):
                    st.copy(k // COPIES, k % COPIES).wait_send()
            (swap_g, swap_d)[g](u).wait_send()
    for cp in puts:
        cp.wait()


def rs(gs, ds):
    scratch = []
    for cut in CUTS:
        us = (cut.units, 2)
        block, width = (cut.n, cut.rows, cut.width), cut.width
        scratch += [
            vmem(us + (3, RING) + block, BF), vmem(us + (2, RING) + block, BF), vmem(us + (RING,) + block, F32), vmem(us + (3,) + block, BF),
            vmem(us + (RING, PAD, width), BF), vmem(us + (RING, PAD, width), F32), vmem(us + (3, PAD, width), BF),
            dma(us + (PHASES * COPIES,)), dma(us + (PHASES * COPIES,)), dma(us + (4,)),
        ]
    n = GATE.units + L
    scratch += [vmem((ZROWS + 8, GATE.width), F32), vmem((PAD + 8, HG), F32)] + [vmem((GATE.units, 16, HG), BF)] * 3
    scratch += [vmem((L, 2, DROWS, HD), BF), vmem((L, DROWS, HD), BF), vmem((5, 8, 128), F32), vmem((10, 8, 128), F32)]
    scratch += [dma((n,)), dma((n,)), dma((10,)), dma((10,)), dma((2 * n + 1,))]
    return call(rs_kernel, [out((GATE.units, 16, FF), BF), out((L, DROWS, D), BF), out((8, 128), F32)], [HBM] * n, scratch, "rs", ident=2)(
        *(t.reshape(RING, RING, 1, ZROWS, HG) for t in gs), *(t.reshape(RING, RING, RING, PAIR, DROWS, HD) for t in ds)
    )


COUNT = 3 * L * D * FF


def adamw_kernel(gg, gd, norm, *refs):
    old, (wg, wu, wd), new, (ng, nd, win, wind, sg, sw, sem) = refs[:6], refs[6:9], refs[9:15], refs[15:]
    i = lax.axis_index("dp")
    start, off = pl.multiple_of(i * ROWS // 8 * 8, 8), i * ROWS % 8
    copies = [pltpu.make_async_copy((wg, wu)[u // L].at[u % L, pl.ds(start, 16), :], win.at[u], sem.at[u]) for u in range(GATE.units)]
    copies.append(pltpu.make_async_copy(wd.at[:, pl.ds(pl.multiple_of(i * DROWS, 8), DROWS), :], wind, sem.at[GATE.units]))
    for cp in copies:
        cp.start()
    factor = jnp.minimum(1.0, 0.5 * lax.rsqrt(jnp.full((1, 1), jnp.sum(norm[...])) / COUNT + 1e-30))
    for cp in copies:
        cp.wait()

    def step(k, w, g):
        g = g * factor
        m = 0.9 * old[k][...] + 0.1 * g
        v = 0.95 * old[k + 3][...] + 0.05 * g * g
        new[k][...], new[k + 3][...] = m, v
        return w - 0.02 * (m * lax.rsqrt(v + 1e-8) + 0.1 * w)

    for k in range(2):
        for l in range(L):
            w = up(win[k * L + l])
            rows = w[0:ROWS]
            for skip in (2, 4, 6):
                rows = jnp.where(off == skip, w[skip : skip + ROWS], rows)
            sw[:, l, :] = rows
            sg[:, l, :] = up(gg[k * L + l])[0:ROWS]
        sw[...] = step(k, sw[...], sg[...])
        for l in range(L):
            ng[k * L + l, 0:ROWS] = sw[:, l, :].astype(BF)
    nd[...] = step(2, up(wind[...]), up(gd[...])).astype(BF)


def adamw(gg, gd, norm, moments, weights):
    flip = lambda k, t: t if k % 3 == 2 else jnp.swapaxes(t, 0, 1)
    moments = [flip(k, t) for k, t in enumerate(moments)]
    outs = [out(t.shape, F32) for t in moments] + [out((GATE.units, 16, FF), BF), out((L, DROWS, D), BF)]
    scratch = [vmem((GATE.units, 16, FF), BF), vmem((L, DROWS, D), BF)] + [vmem((ROWS, L, FF), F32)] * 2 + [dma((GATE.units + 1,))]
    *new, ng, nd = call(adamw_kernel, outs, [VM] * 9 + [HBM] * 3, scratch, "adamw", out_specs=[VM] * 8)(gg, gd, norm, *moments, *weights)
    return [flip(k, t) for k, t in enumerate(new)], ng, nd


class Gathered:
    def __init__(self, here, cut, refs, b, u, s):
        self.here, self.cut, self.refs, self.b, self.u, self.s = here, cut, refs, b, u, s
        self.order = cut.dims(s)[::-1]
        n, first = (HG, s * cut.width) if cut.gate else (HD, 0)
        self.whole = [pl.ds(pl.multiple_of(c * n + first, 128), cut.width) for c in here.at[CORE]]

    def ref(self, at):
        return self.refs[self.u // L].at[(self.u % L,) + at]

    def copy(self, phase, k):
        dim, back = self.order[phase], k % 2
        cols = self.whole[0]
        if k >= 2:
            cols = self.cut.part(self.s, back, cols.start)
        v = self.ref(self.cut.index(self.here, self.s, dim, 0 if k < 2 else 2 * back - 1, self.order[:phase], cols))
        i = phase * 4 + k
        return remote(v, v, self.b[0].at[self.u, self.s, i], self.b[1].at[self.u, self.s, i], self.here.moved(dim, 1 - 2 * back))

    def across(self, r, core=0):
        v = self.ref(self.cut.index(self.here, self.s, self.order[2], r, self.order, self.whole[core]))
        i = PHASES * 4 + r % RING
        return remote(v, v, self.b[0].at[self.u, self.s, i], self.b[1].at[self.u, self.s, i], self.here.moved(CORE))

    def start(self, phase):
        for k in range(2):
            self.copy(phase, k).start()
        if phase == 2:
            self.across(0).start()

    def forward(self, phase):
        for k in range(2):
            self.copy(phase, k).wait_recv()
            self.copy(phase, 2 + k).start()
            if phase == 2:
                self.across(2 * k - 1).start()

    def end(self, phase):
        for k in range(2, 4):
            self.copy(phase, k).wait_recv()
        if phase < 2:
            self.start(phase + 1)
        else:
            self.across(2).start()


def ag_kernel(wg, wd, o0, o1, od, cs, cx, zb, zf, zm, csend, crecv, zsend, zrecv, gsend, grecv, dsend, drecv):
    here = Place()
    (x, y, z, c), other = (steps[0] for steps in here.at), here.moved(CORE)
    meet([here.moved(d, r) for d in (X, Y, Z) for r in (1, -1)] + [other])
    half = lambda which, n: pl.ds(pl.multiple_of(which * n, 128), n)
    mine, theirs = c, 1 - c

    def swap_g(u):
        return remote(wg.at[u, :, half(theirs, HG)], cx.at[u], csend.at[u], crecv.at[u], other)

    def swap_d(l, core, which):
        there = od.at[l, x, y, z, core, :, half(which, HD)]
        return remote(wd.at[l, :, half(theirs, HD)], there, csend.at[GATE.units + l], crecv.at[GATE.units + l], other)

    for u in range(GATE.units):
        swap_g(u).start()
    for l in range(L):
        swap_d(l, c, theirs).start()
        od[l, x, y, z, c, :, half(mine, HD)] = wd[l, :, half(mine, HD)]

    def zcopy(s, k):
        back = k % 2
        cols = GATE.part(s, back, s * GATE.width) if k >= 2 else pl.ds(s * GATE.width, GATE.width)
        v = zb.at[here.at[Z][0 if k < 2 else (2 * back - 1) % RING], :, cols]
        return remote(v, v, zsend.at[s, k], zrecv.at[s, k], here.moved(Z, 1 - 2 * back))

    for u in range(GATE.units):
        swap_g(u).wait_recv()
        own, got = up(wg[u, :, half(mine, HG)]), up(cx[u])
        for core in range(PAIR):
            row = (u * PAIR + core) * ROWS
            cs[row : row + ROWS] = jnp.where(c == core, own, got)[0:ROWS]
    for s in range(2):
        cols = slice(s * GATE.width, (s + 1) * GATE.width)
        zb[z, :, cols] = cs[:, cols].astype(BF)
        for k in range(2):
            zcopy(s, k).start()
    gate = [Gathered(here, GATE, (o0, o1), (gsend, grecv), u, s) for u in range(GATE.units) for s in range(2)]
    down = [Gathered(here, DOWN, (od,), (dsend, drecv), l, s) for l in range(L) for s in range(2)]
    for l in range(L):
        swap_d(l, 1 - c, mine).wait_recv()
    for st in down:
        st.start(0)
    for s in range(2):
        for k in range(2):
            zcopy(s, k).wait_recv()
            zcopy(s, 2 + k).start()
    for st in down:
        st.forward(0)

    for s in range(2):
        cols = slice(s * GATE.width, (s + 1) * GATE.width)
        for k in range(2, 4):
            zcopy(s, k).wait_recv()
        for i in range(RING):
            zm[...] = up(zb[i, :, cols])
            for u in range(GATE.units):
                n = PAIR * ROWS
                zf[u, i * n : i * n + n] = zm[u * n : u * n + n]
        for st in gate[s::2]:
            (o0, o1)[st.u // L][st.u % L, x, y, 0, :, st.whole[0]] = zf[st.u].astype(BF)
            st.start(1)
    for st in down:
        st.end(0)
    both = gate[: L * 2] + down[:2] + gate[L * 2 :] + down[2:]
    for phase in (1, 2):
        for st in both:
            st.forward(phase)
        for st in both:
            st.end(phase)
    for u in range(GATE.units):
        swap_g(u).wait_send()
    for l in range(L):
        swap_d(l, c, theirs).wait_send()
    for s in range(2):
        for k in range(4):
            zcopy(s, k).wait_send()
    for st in both:
        for phase in range(1 if st.cut.gate else 0, PHASES):
            for k in range(4):
                st.copy(phase, k).wait_send()
        for r in range(RING):
            st.across(r).wait_send()
            st.across(r, 1).wait_recv()


def ag(wg, wd):
    block = (RING, RING, 1, ZROWS, FF)
    outs = [pltpu.VMEM((L,) + block, BF)] * 2 + [pltpu.VMEM((L, RING, RING, RING, PAIR, DROWS, D), BF)]
    n, sems = GATE.units, PHASES * 4 + RING
    scratch = [vmem((ZROWS, HG), F32), vmem((n, 16, HG), BF), vmem((RING, ZROWS, HG), BF), vmem((n, ZROWS, GATE.width), F32), vmem((ZROWS, GATE.width), F32)]
    scratch += [dma((n + L,))] * 2 + [dma((2, 4))] * 2 + [dma((n, 2, sems))] * 2 + [dma((L, 2, sems))] * 2
    return call(ag_kernel, outs, [VM] * 2, scratch, "ag", vmem_limit=5 * 2**20, ident=3, out_specs=[VM] * 3)(wg, wd)


def put_kernel(src, dst, sem):
    copies = [pltpu.make_async_copy(src.at[l], dst.at[l], sem.at[l]) for l in range(L)]
    for cp in copies:
        cp.start()
    for cp in copies:
        cp.wait()


def put(w):
    return call(put_kernel, [out(w.shape, BF)], [VM], [dma((L,))], "put", vmem_limit=2**20)(w)[0]


def normed(h):
    wide = up(h)
    scale = lax.rsqrt(jnp.mean(wide**2, -1, keepdims=True) + 1e-6)
    return (wide * scale).astype(BF), scale


def normed_back(h, scale, da):
    wide, da = up(h), up(da)
    mean = jnp.mean(da * wide, -1, keepdims=True)
    return (da * scale - wide * (scale * scale * scale * mean)).astype(BF)


def mm(a, b, across=0):
    return lax.dot_general(a, b, (((1,), (across,)), ((), ())), preferred_element_type=F32)


def gated(gate, u):
    return (jax.nn.silu(gate) * u).astype(BF)


def gated_back(gate, u, dhid):
    sig = jax.nn.sigmoid(gate)
    d = up(dhid)
    return (d * u * (sig * (1 + gate * (1 - sig)))).astype(BF), (d * (gate * sig)).astype(BF)


def device_step(x, dy, wg, wu, wd, *moments):
    x, dy = x[0], dy[0]
    a0, _ = normed(x)
    g0, u0 = mm(a0, wg[0]), mm(a0, wu[0])
    hid0 = gated(g0, u0)
    h1 = x + mm(hid0, wd[0]).astype(BF)
    a1, s1 = normed(h1)
    g1, u1 = mm(a1, wg[1]), mm(a1, wu[1])
    hid1 = gated(g1, u1)
    dg1, du1 = gated_back(g1, u1, mm(dy, wd[1], 1).astype(BF))
    pg1, pu1, pd1 = dw(a1, dg1, du1, hid1, dy)
    da1 = mm(dg1, wg[1], 1).astype(BF) + mm(du1, wu[1], 1).astype(BF)
    dx1 = dy + normed_back(h1, s1, da1)
    dg0, du0 = gated_back(g0, u0, mm(dx1, wd[0], 1).astype(BF))
    pg0, pu0, pd0 = dw(a0, dg0, du0, hid0, dx1)
    gg, gd, norm = rs((pg0, pg1, pu0, pu1), (pd0, pd1))
    moments, ng, nd = adamw(gg, gd, norm, moments, (wg, wu, wd))
    return (*(put(new).reshape(w.shape) for new, w in zip(ag(ng, nd), (wg, wu, wd))), *moments)


def solution(mesh):
    rows, moment, whole = P(("rep", "dp"), None, None), P(None, "dp", None), P(None, None, None)
    return jax.shard_map(
        device_step,
        mesh=mesh,
        in_specs=(rows,) * 2 + (whole,) * 3 + (moment,) * 6,
        out_specs=(P("rep", None, None),) * 3 + (P("rep", "dp", None),) * 6,
        check_vma=False,
    )
```

```python
import functools

import jax
import jax.numpy as jnp
from jax import lax
from jax.experimental import pallas as pl
from jax.experimental.pallas import tpu as pltpu
from jax.sharding import PartitionSpec as P

BF, F32 = jnp.bfloat16, jnp.float32
T, D, FF = 1024, 1280, 3072
L, RING, PAIR = 2, 4, 2
X, Y, Z, CORE = range(4)
HG, HD = FF // PAIR, D // PAIR
ROWS, DROWS = D // (RING**3 * PAIR), FF // (RING**3 * PAIR)
ZROWS = PAIR * RING * ROWS
NT = 256
WIDE = 512
PAD = 24
MOST = 67043328
HBM, VM = pl.BlockSpec(memory_space=pltpu.HBM), pl.BlockSpec(memory_space=pltpu.VMEM)
dma, vmem = pltpu.SemaphoreType.DMA, pltpu.VMEM
out = jax.ShapeDtypeStruct
ALL, BOTH = slice(None), range(2)
PAIR_SEM, PAIRS_SEM = dma((2,)), dma((2, 2))


class Place:
    def __init__(self):
        i = lax.axis_index("dp")
        chip, core = lax.div(i, PAIR), lax.rem(i, PAIR)
        self.at = [[lax.div(chip, RING**2)], [lax.rem(lax.div(chip, RING), RING)], [lax.rem(chip, RING)], [core, 1 - core]]
        for steps in self.at[:CORE]:
            steps += [lax.rem(steps[0] + r, RING) for r in range(1, RING)]
        self.peers = {}

    def moved(self, dim, by=1):
        by %= len(self.at[dim])
        if (dim, by) not in self.peers:
            x, y, z, core = (steps[by if d == dim else 0] for d, steps in enumerate(self.at))
            self.peers[dim, by] = {"dp": ((x * RING + y) * RING + z) * PAIR + core}
        return self.peers[dim, by]


def meet(peers):
    barrier = pltpu.get_barrier_semaphore()
    for peer in peers:
        pl.semaphore_signal(barrier, inc=1, device_id=peer)
    pl.semaphore_wait(barrier, len(peers))


def remote(src, dst, send, recv, peer):
    return pltpu.make_async_remote_copy(src, dst, send, recv, device_id=peer)


def up(v):
    return v.astype(F32)


def call(kernel, outs, ins, scratch, name, vmem_limit=MOST, ident=None, out_specs=None, **more):
    return pl.pallas_call(
        kernel,
        out_shape=outs,
        in_specs=ins,
        out_specs=out_specs or [HBM] * len(outs),
        scratch_shapes=scratch,
        compiler_params=pltpu.CompilerParams(collective_id=ident, has_side_effects=ident is not None, vmem_limit_bytes=vmem_limit),
        name=name,
        **more,
    )


def odd(i):
    return lax.rem(i, 2)


def tiled(n, body, hooks=(), base=0):
    def one(i, _):
        body(i)
        for k, hook in hooks:
            pl.when(base + i == k)(hook)
        return _

    lax.fori_loop(0, n, one, 0)


class Loaded:
    def __init__(self, n, src, buf, sem):
        self.n, self.src, self.buf, self.sem = n, src, buf, sem

    def copy(self, i):
        slot = odd(i)
        return pltpu.make_async_copy(self.src(i), self.buf.at[slot], self.sem.at[slot])

    def start(self):
        self.copy(jnp.int32(0)).start()

    def ready(self, i):
        pl.when(i + 1 < self.n)(lambda: self.copy(i + 1).start())
        self.copy(i).wait()

    def take(self, i):
        self.ready(i)
        return odd(i)


def mm(a, b, across=0):
    return lax.dot_general(a, b, (((1,), (across,)), ((), ())), preferred_element_type=F32)


def tn(a, b):
    return lax.dot_general(a, b, (((0,), (0,)), ((), ())), preferred_element_type=F32).astype(BF)


def at(i, n, base=0):
    return pl.ds(pl.multiple_of(base + i * n, 128), n)


def fetch(pairs, sem):
    copies = [pltpu.make_async_copy(src, dst, sem.at[i]) for i, (src, dst) in enumerate(pairs)]
    for cp in copies:
        cp.start()
    return copies


class Cut:
    def __init__(self, gate):
        self.gate = gate
        self.width = HG // 2 if gate else HD
        self.n, self.rows = (1, ZROWS) if gate else (RING, DROWS)

    def dims(self, s):
        return (s, 1 - s, Z) if self.gate else (Z, s, 1 - s)

    def part(self, s, h, base=0):
        first = 384 if self.gate or s == 0 else 256
        return pl.ds(base + first, self.width - first) if h else pl.ds(base, first)

    def index(self, here, s, dim, r, done, cols):
        at = [here.at[d][r % RING] if d == dim else ALL if d in done else here.at[d][0] for d in (X, Y, Z)]
        return (at[X], at[Y]) + ((ALL,) if self.gate else (at[Z], s)) + (ALL, cols)


GATE, DOWN = Cut(True), Cut(False)


def ahead(k):
    return 1 if k in (0, 3, 4) else -1


PART = T // 4


def in_pairs(body):
    def both(i):
        for k in BOTH:
            body(at(2 * i + k, PART))

    tiled(T // (2 * PART), both)


def normed(src, dst):
    def rows(i):
        r = at(i, PART)
        wide = up(src[r])
        dst[r] = (wide * lax.rsqrt(jnp.mean(wide**2, -1, keepdims=True) + 1e-6)).astype(BF)

    tiled(T // PART, rows)


def gated(gate, u):
    sig = jax.nn.sigmoid(gate)
    silu = gate * sig
    return (silu * u).astype(BF), u * (sig * (1 + gate * (1 - sig))), silu


class Stored:
    def __init__(self, dst, buf, sem):
        self.dst, self.buf, self.sem = dst, buf, sem

    def copy(self, i):
        slot = odd(i)
        return pltpu.make_async_copy(self.buf.at[slot], self.dst(i), self.sem.at[slot])

    def free(self, i):
        pl.when(i >= 2)(lambda: self.copy(i - 2).wait())

    def end(self, n):
        for i in (n - 2, n - 1):
            self.copy(jnp.int32(i)).wait()


HALVES = vmem((2, 2, D, WIDE), BF)
STATES = vmem((T, D), BF)


def forward_kernel(x, dy, wg, wu, wd, oa0, ohid0, ofg, ofu, oh1, oa1, ohid1, od1, vx, va, vhid, vdy, sem, osem, hsem):
    n = FF // WIDE
    x_here, dy_here = fetch([(x, vx), (dy, vdy)], sem)
    wide = lambda ref, l: lambda i: ref.at[l, :, at(i, WIDE)]

    def put(i):
        return pltpu.make_async_copy(vhid.at[:, at(i, WIDE)], ohid0.at[:, at(i, WIDE)], hsem.at[i])

    def first(vw, wsem, vo, vsem):
        tiles = [Loaded(n, wide(w, 0), vw.at[k], wsem.at[k]) for k, w in enumerate((wg, wu))]
        outs = [Stored(lambda i, o=o: o.at[:, at(i, WIDE)], vo.at[k], vsem.at[k]) for k, o in enumerate((ofg, ofu))]
        for t in tiles:
            t.start()
        x_here.wait()
        normed(vx, va)
        a_out, = fetch([(va, oa0)], osem)

        def body(i):
            slot, _ = [t.take(i) for t in tiles]
            for o in outs:
                o.free(i)

            def rows(r):
                vhid[r, at(i, WIDE)], *factors = gated(*(mm(va[r], vw[k, slot]) for k in BOTH))
                for k in BOTH:
                    vo[k, slot, r] = factors[k]

            in_pairs(rows)
            put(i).start()
            for o in outs:
                o.copy(i).start()

        tiled(n, body)
        for o in outs:
            o.end(n)
        a_out.wait()

    pl.run_scoped(first, HALVES, PAIRS_SEM, vmem((2, 2, T, WIDE), F32), PAIRS_SEM)

    def second(vw, wsem):
        tiles = Loaded(D // NT, lambda i: wd.at[0, :, at(i, NT)], vw, wsem)
        tiles.start()

        def body(i):
            slot, cols = tiles.take(i), at(i, NT)

            def rows(r):
                vx[r, cols] = (up(vx[r, cols]) + up(mm(vhid[r], vw[slot]).astype(BF))).astype(BF)

            in_pairs(rows)

        tiled(D // NT, body)

    pl.run_scoped(second, vmem((2, FF, NT), BF), PAIR_SEM)
    for i in range(n):
        put(i).wait()

    def third(vw, wsem, vd, dsem, vo, vsem):
        tiles = [Loaded(n, wide(w, 1), vw.at[k], wsem.at[k]) for k, w in enumerate((wg, wu))]
        tiles.append(Loaded(n, lambda i: wd.at[1, at(i, WIDE), :], vd, dsem))
        outs = [Stored(lambda i, o=o: o.at[:, at(i, WIDE)], vo.at[k], vsem.at[k]) for k, o in enumerate((od1.at[0], od1.at[1], ohid1))]
        for t in tiles:
            t.start()
        normed(vx, va)
        kept = fetch([(vx, oh1), (va, oa1)], osem)
        dy_here.wait()

        def body(i):
            slot, *_ = [t.take(i) for t in tiles]
            for o in outs:
                o.free(i)

            def rows(r):
                hid, *factors = gated(*(mm(va[r], vw[k, slot]) for k in BOTH))
                dhid = up(mm(vdy[r], vd[slot], 1).astype(BF))
                vo[2, slot, r] = hid
                for k in BOTH:
                    vo[k, slot, r] = (dhid * factors[k]).astype(BF)

            in_pairs(rows)
            for o in outs:
                o.copy(i).start()

        tiled(n, body)
        for o in outs:
            o.end(n)
        for cp in kept:
            cp.wait()

    pl.run_scoped(third, HALVES, PAIRS_SEM, vmem((2, WIDE, D), BF), PAIR_SEM, vmem((3, 2, T, WIDE), BF), dma((3, 2)))


def forward(x, dy, wg, wu, wd):
    states, hidden = out((T, D), BF), out((T, FF), BF)
    outs = [states, hidden, out((T, FF), F32), out((T, FF), F32), states, states, hidden, out((2, T, FF), BF)]
    scratch = [STATES] * 2 + [vmem((T, FF), BF), STATES, PAIR_SEM, PAIR_SEM, dma((FF // WIDE,))]
    return call(forward_kernel, outs, [HBM] * 5, scratch, "forward")(x, dy, wg, wu, wd)


SUM, OWN, GOT = range(3)
TILES = 6
TILE = FF // TILES
DOWN_SCRATCH = [vmem((TILES, TILE, HD), BF)] + [dma((TILES,))] * 2 + [dma((GOT + 1, TILES))]
HIDDEN = [vmem((2, T, TILE), BF), PAIR_SEM, vmem((TILES, PAIR, TILE, HD), BF)]
BLOCKS = (RING, RING, 1, ZROWS)
GATE_SCRATCH = [vmem((2, 2) + BLOCKS + (GATE.width,), BF)] * 3 + [PAIRS_SEM] * 2
GATE_SUMS, DOWN_SUMS = out((GOT + 1, 2) + BLOCKS + (HG,), BF), out((GOT + 1, FF, HD), BF)


class DownProduct:
    def __init__(self, here, hid, hbuf, hsem, halves, got, send, recv, outsem):
        self.here, self.halves, self.got, self.send, self.recv, self.outsem = here, halves, got, send, recv, outsem
        self.hidden = Loaded(TILES, lambda i: hid.at[:, at(i, TILE)], hbuf, hsem)
        self.hidden.start()

    def swap(self, i):
        _, theirs = self.here.at[CORE]
        return remote(self.halves.at[i, theirs], self.got.at[i], self.send.at[i], self.recv.at[i], self.here.moved(CORE))

    def put(self, od, i):
        mine, theirs = self.here.at[CORE]
        srcs = self.halves.at[i, theirs], self.halves.at[i, mine], self.got.at[i]
        return [pltpu.make_async_copy(src, od.at[k, at(i, TILE), :], self.outsem.at[k, i]) for k, src in enumerate(srcs)]

    def run(self, dy, od, hooks=()):
        mine, theirs = self.here.at[CORE]

        def add(i):
            self.swap(i).wait()
            self.halves[i, theirs] = (up(self.got[i]) + up(self.halves[i, mine])).astype(BF)
            for cp in self.put(od, i):
                cp.start()

        def body(i):
            full = tn(self.hidden.buf[self.hidden.take(i)], dy[...])
            for half in BOTH:
                self.halves[i, half] = full[:, half * HD : (half + 1) * HD]
            self.swap(i).start()
            pl.when(i > 0)(lambda: add(i - 1))

        tiled(TILES, body, hooks)
        add(TILES - 1)
        for i in range(TILES):
            for cp in self.put(od, i):
                cp.wait()


class GateProducts:
    def __init__(self, here, d, buf, sem, total, own, got, send, recv):
        self.here, self.sems = here, (send, recv)
        self.terms = total, own, got

        def src(i):
            t, (mine, theirs) = lax.rem(i, 4), here.at[CORE]
            return d.at[lax.div(i, 4), :, at(odd(i), GATE.width, jnp.where(t < 2, theirs, mine) * HG)]

        self.tiles = Loaded(8, src, buf, sem)
        self.tiles.start()

    def swap(self, w, t):
        send, recv = self.sems
        return remote(self.terms[SUM].at[w, t], self.terms[GOT].at[w, t], send.at[w, t], recv.at[w, t], self.here.moved(CORE))

    def put(self, og, sem, w, t):
        return [pltpu.make_async_copy(v.at[w, t], og.at[k, w, :, :, :, :, at(t, GATE.width)], sem.at[k, w, t]) for k, v in enumerate(self.terms)]

    def run(self, a, hooks=(), after=lambda w, t: None):
        total, own, got = self.terms

        def product(i):
            return tn(a[...], self.tiles.buf[self.tiles.take(i)]).reshape(BLOCKS + (GATE.width,))

        def matrix(w, _):
            def theirs(t):
                total[w, t] = product(4 * w + t)
                self.swap(w, t).start()

            def mine(t):
                own[w, t] = product(4 * w + 2 + t)
                self.swap(w, t).wait()
                total[w, t] = (up(got[w, t]) + up(own[w, t])).astype(BF)
                after(w, t)

            tiled(2, theirs, hooks, 4 * w)
            tiled(2, mine, hooks, 4 * w + 2)
            return _

        lax.fori_loop(0, 2, matrix, 0)


COLUMNS = [vmem((2, T, GATE.width), BF), PAIR_SEM]


def dw_kernel(a, d, hid, dy, og, od, va, vy, sem, gout, *refs):
    here = Place()
    n = len(HIDDEN + DOWN_SCRATCH)
    down = DownProduct(here, hid, *refs[:n])
    dy_here, a_here = fetch([(dy, vy), (a, va)], sem)
    gates = GateProducts(here, d, *refs[n:])
    meet([here.moved(CORE)])

    def put(w, t):
        for cp in gates.put(og, gout, w, t):
            cp.start()

    dy_here.wait()
    down.run(vy, od)
    a_here.wait()
    gates.run(va, after=put)
    for w in BOTH:
        for t in BOTH:
            for cp in gates.put(og, gout, w, t):
                cp.wait()


def dw(a, d, hid, dy):
    scratch = [STATES] * 2 + [PAIR_SEM, dma((GOT + 1, 2, 2))] + HIDDEN + DOWN_SCRATCH + COLUMNS + GATE_SCRATCH
    return call(dw_kernel, [GATE_SUMS, DOWN_SUMS], [HBM] * 4, scratch, "dw", ident=1)(a, d, hid, dy)


PHASES, COPIES = 3, 6
NAMES = ("r1", "o1", "k2", "r2", "t3", "k3", "r3", "send", "recv", "own")


class Summed:
    def __init__(self, here, cut, src, b, u, s):
        self.here, self.cut, self.src, self.us, self.s, self.dims = here, cut, src, (u, s), s, cut.dims(s)
        self.got, self.kept = [b[k] for k in ("r1", "r2", "r3")], [b[k] for k in ("o1", "k2", "k3")]
        self.t3, self.sems, self.direct = b["t3"], (b["send"], b["recv"], b["own"]), isinstance(src, tuple)

    def block(self, phase, r, cols=ALL, first=()):
        dim = self.dims[phase]
        i = self.here.at[dim][r % RING]
        if phase == 2:
            return self.us + first + (i, ALL, cols)
        second = phase == 1 and not self.cut.gate and self.s
        return self.us + first + ((ALL, i) if second else (i, ALL)) + (ALL, cols)

    def first(self, kind, r, h):
        if self.direct:
            ref, lead, base = self.src[kind], self.us, 0
        else:
            ref, lead, base = self.src, (kind,) + (self.us[:1] if self.cut.gate else ()), self.s * self.cut.width if self.cut.gate else 0
        return ref.at[lead + self.cut.index(self.here, self.s, self.dims[0], r, self.dims, self.cut.part(self.s, h, base))]

    def term(self, n, cols=ALL, r=0):
        if self.direct:
            i = self.here.at[self.dims[0]][r % RING]
            at_, terms = [self.us + ((n, i) if self.s else (i, n)) + (ALL, ALL, cols)] * 2, self.src[OWN:]
        else:
            at_, terms = [self.us + (k, n, ALL, ALL, cols) for k in BOTH], [self.kept[0]] * 2
        return sum(up(ref[i]) for ref, i in zip(terms, at_))

    def at(self, phase, kind, cols=ALL):
        return self.us + (kind,) + (ALL,) * (PHASES - phase) + (cols,)

    def copy(self, phase, k):
        kind, h = k // 2, k % 2
        cols = self.cut.part(self.s, h)
        got = self.got[phase]
        r = (2, -ahead(h), 0)[kind]
        if kind == 2:
            src = got.at[self.at(phase, 0, cols)]
        elif phase == 0:
            src = self.first(SUM, r, h)
        elif phase == 1:
            src = self.got[0].at[self.block(1, r, cols, (2,))]
        else:
            src = self.t3.at[self.block(2, r, cols)]
        send, recv, _ = self.sems
        i = self.us + (phase * COPIES + k,)
        return remote(src, got.at[self.at(phase, kind, cols)], send.at[i], recv.at[i], self.here.moved(self.dims[phase], ahead(k)))

    def own(self, k):
        kind, h = k // 2, k % 2
        cols, copies = self.cut.part(self.s, h), []
        for term in () if self.direct else BOTH:
            dst = self.kept[0].at[self.us + (term,) + (ALL,) * PHASES + (cols,)]
            copies.append(pltpu.make_async_copy(self.first(OWN + term, 0 if kind else ahead(h), h), dst, self.sems[2].at[self.us + (k, term)]))
        return copies

    def start(self, part):
        for h in BOTH:
            self.copy(0, 2 * part + h).start()
            for cp in [] if part else self.own(h):
                cp.start()

    def arrive(self, ks):
        for k in ks:
            for cp in self.own(k):
                cp.wait()

    def pass_on(self, phase):
        got, kept = self.got[phase], self.kept[phase]
        for h in BOTH:
            self.copy(phase, h).wait_recv()
            cols = self.cut.part(self.s, h)
            if phase:
                i = self.at(phase, 0, cols)
                got[i] = (up(got[i]) + kept[self.block(phase, ahead(h), cols)]).astype(BF)
            else:
                self.arrive([h])

                def add(n):
                    i = self.us + (0, n, ALL, ALL, cols)
                    got[i] = (up(got[i]) + self.term(n, cols, ahead(h))).astype(BF)

                tiled(RING, add)
            self.copy(phase, 4 + h).start()
        for h in () if phase else BOTH:
            for cp in self.own(2 + h):
                cp.start()

    def finish(self, phase):
        for k in range(2, COPIES):
            self.copy(phase, k).wait_recv()
        got, kept = self.got[phase], self.kept[phase]
        if phase:
            return kept[self.block(phase, 0)] + up(got[self.us + (2,)]) + up(got[self.us + (1,)])
        self.arrive((2, 3))

        def add(n):
            total = self.term(n) + up(got[self.us + (2, n)]) + up(got[self.us + (1, n)])
            self.kept[1][self.us + (n,)] = total
            got[self.us + (2, n)] = total.astype(BF)

        tiled(RING, add)

    def starts(self, phase):
        for k in range(4):
            self.copy(phase, k).start()


class Sums:
    def __init__(self, here, og, od, refs):
        self.here = here
        n = len(NAMES)
        bufs = [dict(zip(NAMES, refs[i : i + n])) for i in (0, n)]
        self.f3, self.f4, self.ce, self.cr, self.co, self.fd, self.dr, self.csend, self.crecv, self.putsem = refs[2 * n :]
        self.gate, self.upper = ([Summed(here, GATE, og, bufs[0], u, s) for s in BOTH] for u in BOTH)
        self.down = [Summed(here, DOWN, od, bufs[1], 0, s) for s in BOTH]
        self.puts = []
        self.f3[ZROWS : ZROWS + 8] = jnp.zeros((8, GATE.width), F32)
        self.f4[PAD : PAD + 8] = jnp.zeros((8, HG), F32)

    def begin(self, streams):
        for part in BOTH:
            for st in streams:
                st.start(part)

    def second(self, st):
        total = st.finish(1)
        if st.cut.gate:
            self.f3[0:ZROWS] = total[0]
            for i in range(RING):
                rows = self.f3[i * PAIR * ROWS : i * PAIR * ROWS + PAD]
                st.kept[2][st.us + (i,)] = rows
                st.t3[st.us + (i,)] = rows.astype(BF)
        else:
            st.kept[2][st.us] = total
            st.t3[st.us] = total.astype(BF)

    def step(self, n, *streams):
        for st in streams:
            if n % 2 == 0:
                st.pass_on(n // 2)
            else:
                if n == 1:
                    st.finish(0)
                else:
                    self.second(st)
                st.starts(n // 2 + 1)

    def swap(self, u):
        src, dst = (self.fd.at[self.here.at[CORE][1]], self.dr) if u == 2 else (self.ce.at[u], self.cr.at[u])
        return remote(src, dst, self.csend.at[u], self.crecv.at[u], self.here.moved(CORE))

    def last(self, u):
        if u == 2:
            for st in self.down:
                self.fd[st.s] = st.finish(2).astype(BF)
            parts = [up(self.fd[s]) for s in BOTH]
        else:
            for st in self.upper if u else self.gate:
                self.f4[0:PAD, st.s * GATE.width : (st.s + 1) * GATE.width] = st.finish(2)
            low, high = self.f4[0:16], self.f4[ROWS : ROWS + 16]
            first = self.here.at[CORE][0] == 0
            self.co[u] = jnp.where(first, low, high).astype(BF)
            self.ce[u] = jnp.where(first, high, low).astype(BF)
            valid = lax.broadcasted_iota(jnp.int32, (PAD, HG), 0) < PAIR * ROWS
            parts = [jnp.where(valid, up(self.f4[0:PAD].astype(BF)), 0.0)]
        self.swap(u).start()
        return sum(squares(v) for v in parts)

    def put(self, src, dst):
        self.puts.append(pltpu.make_async_copy(src, dst, self.putsem.at[len(self.puts)]))
        self.puts[-1].start()

    def results(self, gg, gd):
        mine, theirs = self.here.at[CORE]
        for u in range(3):
            n, dst = (HD, gd) if u == 2 else (HG, gg.at[u])
            self.put(self.fd.at[mine] if u == 2 else self.co.at[u], dst.at[:, at(mine, n)])
            self.swap(u).wait()
            self.put(self.dr if u == 2 else self.cr.at[u], dst.at[:, at(theirs, n)])

    def drain(self):
        for st in self.down + self.gate + self.upper:
            for k in range(PHASES * COPIES):
                st.copy(k // COPIES, k % COPIES).wait_send()
        for cp in self.puts:
            cp.wait()


def squares(v):
    v = v * v
    rows = sum(v[i : i + 8] for i in range(0, v.shape[0], 8))
    return sum(rows[:, i : i + 128] for i in range(0, v.shape[1], 128))


LANES = vmem((8, 128), F32)


def sums_scratch(direct):
    scratch = []
    for cut, units in ((GATE, 2), (DOWN, 1)):
        us, block, width = (units, 2), (cut.n, cut.rows, cut.width), cut.width
        terms = LANES if direct and cut.gate else vmem(us + (2, RING) + block, BF)
        scratch += [vmem(us + (3, RING) + block, BF), terms, vmem(us + (RING,) + block, F32), vmem(us + (3,) + block, BF)]
        scratch += [vmem(us + (RING, PAD, width), t) for t in (BF, F32)] + [vmem(us + (3, PAD, width), BF)]
        scratch += [dma(us + (PHASES * COPIES,))] * 2 + [dma(us + (4, 2))]
    scratch += [vmem((ZROWS + 8, GATE.width), F32), vmem((PAD + 8, HG), F32)] + [vmem((2, 16, HG), BF)] * 3
    return scratch + [vmem((2, DROWS, HD), BF), vmem((DROWS, HD), BF)] + [dma((3,))] * 2 + [dma((7,))]


ROWS_OUT = [out((2, 16, FF), BF), out((DROWS, D), BF), out((8, 128), F32)]
DOWN_BLOCKS = (GOT + 1, RING, RING, RING, PAIR, DROWS, HD)


def all_peers(here):
    return [here.moved(d, r) for d in (X, Y, Z) for r in range(1, RING)] + [here.moved(CORE)]


def over_all(here, total, nb, nr, send, recv):
    n = 0
    for stage, dim in enumerate((CORE, Z, Y, X)):
        nb[stage] = total
        copies = []
        for r in range(1, len(here.at[dim])):
            copies.append(remote(nb.at[stage], nr.at[n], send.at[n], recv.at[n], here.moved(dim, r)))
            copies[-1].start()
            n += 1
        for i, cp in enumerate(copies):
            cp.wait()
            total = total + nr[n - len(copies) + i]
    return total


def back_kernel(d, h1, dy, wg, wu, wd, by_gate, by_up, hid, pg, pd, od0, opd, gg, gd, osq, dx, nb, sem, *refs):
    here = Place()
    n = len(DOWN_SCRATCH)
    sums = Sums(here, pg, pd, refs[n:])
    meet(all_peers(here))
    step = lambda n, streams: lambda: sums.step(n, *streams)
    early, late = zip(sums.down, sums.gate[:1] + sums.upper[:1], sums.gate[1:] + sums.upper[1:])
    sums.begin(early + late)

    def states(vd, vw, wsem):
        n = D // NT
        tiles = [Loaded(n, lambda i, w=w: w.at[1, at(i, NT), :], vw.at[k], wsem.at[k]) for k, w in enumerate((wg, wu))]
        loads = []
        for k in BOTH:
            loads += fetch([(d.at[k], vd.at[k])], sem.at[pl.ds(k, 1)])
            tiles[k].start()

        def body(i):
            k, i = lax.div(i, n), lax.rem(i, n)
            for which in BOTH:
                pl.when(k == which)(lambda: tiles[which].ready(i))
            before = jnp.where(k == 0, 0.0, up(dx[:, at(i, NT)]))
            dx[:, at(i, NT)] = (before + up(mm(vd[k], vw[k, odd(i)], 1).astype(BF))).astype(BF)

        hooks = [(n - 1, loads[1].wait), (n // 2, step(0, early)), (n + 1, step(0, late))]
        loads[0].wait()
        tiled(2 * n, body, hooks)

    pl.run_scoped(states, vmem((2, T, FF), BF), vmem((2, 2, NT, FF), BF), PAIRS_SEM)

    def norm_back(vh, vy):
        for cp in fetch([(h1, vh), (dy, vy)], sem):
            cp.wait()

        def rows(i):
            r = at(i, NT)
            wide, da = up(vh[r]), up(dx[r])
            scale = lax.rsqrt(jnp.mean(wide**2, -1, keepdims=True) + 1e-6)
            mean = jnp.mean(da * wide, -1, keepdims=True)
            back = (da * scale - wide * (scale * scale * scale * mean)).astype(BF)
            dx[r] = (up(vy[r]) + up(back)).astype(BF)

        tiled(T // NT, rows)

    pl.run_scoped(norm_back, STATES, STATES)

    def hidden_back(vw, wsem, vf, fsem, vo, outsem):
        n = FF // WIDE
        tiles = [Loaded(n, lambda i: wd.at[0, at(i, WIDE), :], vw, wsem)]
        tiles += [Loaded(n, lambda i, f=f: f.at[:, at(i, WIDE)], vf.at[k], fsem.at[k]) for k, f in enumerate((by_gate, by_up))]
        outs = [Stored(lambda i, k=k: od0.at[k, :, at(i, WIDE)], vo.at[k], outsem.at[k]) for k in BOTH]
        for t in tiles:
            t.start()

        def body(i):
            slot, *_ = [t.take(i) for t in tiles]
            for o in outs:
                o.free(i)

            def rows(r):
                dhid = up(mm(dx[r], vw[slot], 1).astype(BF))
                for k in BOTH:
                    vo[k, slot, r] = (dhid * vf[k, slot, r]).astype(BF)

            in_pairs(rows)
            for o in outs:
                o.copy(i).start()

        tiled(n, body, [(2, step(1, early)), (5, step(1, late))])
        for o in outs:
            o.end(n)

    pl.run_scoped(hidden_back, vmem((2, WIDE, D), BF), PAIR_SEM, vmem((2, 2, T, WIDE), F32), PAIRS_SEM, vmem((2, 2, T, WIDE), BF), PAIRS_SEM)

    def last(*tile_refs):
        steps = [step(n, streams) for n in (2, 3, 4) for streams in (early, late)]
        DownProduct(here, hid, *tile_refs, *refs[:n]).run(dx, opd, list(enumerate(steps)))

    pl.run_scoped(last, *HIDDEN)
    nb[...] = sum(sums.last(u) for u in (2, 0, 1))
    sums.results(gg, gd)
    sums.put(nb, osq)
    sums.drain()


def back(*args):
    *ins, pg, pd = args
    outs = [out((2, T, FF), BF), DOWN_SUMS] + ROWS_OUT
    scratch = [STATES, LANES, PAIR_SEM] + DOWN_SCRATCH + sums_scratch(False)
    return call(back_kernel, outs, [HBM] * len(args), scratch, "back", ident=2)(*ins, pg, pd.reshape(DOWN_BLOCKS))


def end_kernel(a, d, pd, sq, gg, gd, osq, va, vsq, nb, nr, nsend, nrecv, sem, *refs):
    here = Place()
    n = len(COLUMNS + GATE_SCRATCH)
    gates = GateProducts(here, d, *refs[:n])
    sums = Sums(here, gates.terms, pd, refs[n:])
    a_here, sq_here = fetch([(a, va), (sq, vsq)], sem)
    meet(all_peers(here))
    sums.begin(sums.down)
    a_here.wait()
    (d0, d1), (g0, g1), (u0, u1) = sums.down, sums.gate, sums.upper

    def begin(new, *old):
        sums.begin([new])
        sums.step(0, *old)

    hooks = {2: lambda: begin(g0, d0), 3: lambda: begin(g1, d1), 5: lambda: sums.step(0, g0, g1), 6: lambda: sums.begin([u0])}
    gates.run(va, hooks.items())
    sums.begin([u1])
    sums.step(1, g0, d0, g1)
    sums.step(0, u0)
    sums.step(1, d1)
    sums.step(0, u1)
    for n in (2, 3):
        sums.step(n, g0, d0, g1, d1)
    sums.step(1, u0, u1)
    sums.step(4, g0, d0, g1, d1)
    sums.step(2, u0, u1)
    total = sums.last(2) + sums.last(0)
    for n in (3, 4):
        sums.step(n, u0, u1)
    total += sums.last(1)
    sq_here.wait()
    nb[4] = over_all(here, total + vsq[...], nb, nr, nsend, nrecv)
    sums.put(nb.at[4], osq)
    sums.results(gg, gd)
    sums.drain()


def end(a, d, pd, sq):
    scratch = [STATES, LANES, vmem((5, 8, 128), F32), vmem((10, 8, 128), F32)] + [dma((10,))] * 2 + [PAIR_SEM]
    scratch += COLUMNS + GATE_SCRATCH + sums_scratch(True)
    return call(end_kernel, ROWS_OUT, [HBM] * 4, scratch, "end", ident=4)(a, d, pd.reshape(DOWN_BLOCKS), sq)


COUNT = 3 * L * D * FF


def adamw_kernel(gg0, gg1, gd0, gd1, norm, *refs):
    old, (wg, wu, wd), new, (ng, nd, win, wind, sg, sw, sem) = refs[:6], refs[6:9], refs[9:15], refs[15:]
    i = lax.axis_index("dp")
    start, off = pl.multiple_of(i * ROWS // 8 * 8, 8), i * ROWS % 8
    copies = [pltpu.make_async_copy((wg, wu)[u // L].at[u % L, pl.ds(start, 16), :], win.at[u], sem.at[u]) for u in range(PAIR * L)]
    copies.append(pltpu.make_async_copy(wd.at[:, pl.ds(pl.multiple_of(i * DROWS, 8), DROWS), :], wind, sem.at[PAIR * L]))
    for cp in copies:
        cp.start()
    factor = jnp.minimum(1.0, 0.5 * lax.rsqrt(jnp.full((1, 1), jnp.sum(norm[...])) / COUNT + 1e-30))
    for cp in copies:
        cp.wait()

    def step(k, w, g):
        g = g * factor
        m = 0.9 * old[k][...] + 0.1 * g
        v = 0.95 * old[k + 3][...] + 0.05 * g * g
        new[k][...], new[k + 3][...] = m, v
        return w - 0.02 * (m * lax.rsqrt(v + 1e-8) + 0.1 * w)

    for k in BOTH:
        for l in BOTH:
            w = up(win[k * L + l])
            rows = w[0:ROWS]
            for skip in (2, 4, 6):
                rows = jnp.where(off == skip, w[skip : skip + ROWS], rows)
            sw[:, l, :] = rows
            sg[:, l, :] = up((gg0, gg1)[l][k])[0:ROWS]
        sw[...] = step(k, sw[...], sg[...])
        for l in BOTH:
            ng[k * L + l, 0:ROWS] = sw[:, l, :].astype(BF)
    nd[...] = step(2, up(wind[...]), jnp.stack([up(gd0[...]), up(gd1[...])])).astype(BF)


def adamw(sums, norm, moments, weights):
    weights = [pltpu.with_memory_space_constraint(w, pltpu.HBM) for w in weights]
    flip = lambda k, t: t if k % 3 == 2 else jnp.swapaxes(t, 0, 1)
    moments = [flip(k, t) for k, t in enumerate(moments)]
    outs = [out(t.shape, F32) for t in moments] + [vmem((PAIR * L, 16, FF), BF), vmem((L, DROWS, D), BF)]
    scratch = [vmem((PAIR * L, 16, FF), BF), vmem((L, DROWS, D), BF)] + [vmem((ROWS, L, FF), F32)] * 2 + [dma((PAIR * L + 1,))]
    *new, ng, nd = call(adamw_kernel, outs, [VM] * 11 + [HBM] * 3, scratch, "adamw", MOST - 5 * 2**17, out_specs=[VM] * 8)(*sums, norm, *moments, *weights)
    return [flip(k, t) for k, t in enumerate(new)], ng, nd


class Gathered:
    def __init__(self, here, cut, refs, b, u, s):
        self.here, self.cut, self.refs, self.b, self.u, self.s = here, cut, refs, b, u, s
        self.order = cut.dims(s)[::-1]
        n, first = (HG, s * cut.width) if cut.gate else (HD, 0)
        self.whole = [pl.ds(pl.multiple_of(c * n + first, 128), cut.width) for c in here.at[CORE]]

    def ref(self, at):
        return self.refs[self.u // L].at[(self.u % L,) + at]

    def copy(self, phase, k):
        dim, back = self.order[phase], k % 2
        cols = self.whole[0]
        if k >= 2:
            cols = self.cut.part(self.s, back, cols.start)
        v = self.ref(self.cut.index(self.here, self.s, dim, 0 if k < 2 else 2 * back - 1, self.order[:phase], cols))
        i = phase * 4 + k
        return remote(v, v, self.b[0].at[self.u, self.s, i], self.b[1].at[self.u, self.s, i], self.here.moved(dim, 1 - 2 * back))

    def across(self, r, core=0):
        v = self.ref(self.cut.index(self.here, self.s, self.order[2], r, self.order, self.whole[core]))
        i = PHASES * 4 + r % RING
        return remote(v, v, self.b[0].at[self.u, self.s, i], self.b[1].at[self.u, self.s, i], self.here.moved(CORE))

    def start(self, phase):
        for k in BOTH:
            self.copy(phase, k).start()
        if phase == 2:
            self.across(0).start()

    def forward(self, phase):
        for k in BOTH:
            self.copy(phase, k).wait_recv()
            self.copy(phase, 2 + k).start()
            if phase == 2:
                self.across(2 * k - 1).start()

    def end(self, phase):
        for k in BOTH:
            self.copy(phase, 2 + k).wait_recv()
        if phase < 2:
            self.start(phase + 1)
        else:
            self.across(2).start()


def ag_kernel(wg, wd, o0, o1, od, cs, cx, zb, zf, zm, csend, crecv, zsend, zrecv, gsend, grecv, dsend, drecv):
    here = Place()
    (x, y, z, c), other = (steps[0] for steps in here.at), here.moved(CORE)
    meet([here.moved(d, r) for d in (X, Y, Z) for r in (1, -1)] + [other])
    half = lambda which, n: pl.ds(pl.multiple_of(which * n, 128), n)
    mine, theirs = c, 1 - c

    def swap_g(u):
        return remote(wg.at[u, :, half(theirs, HG)], cx.at[u], csend.at[u], crecv.at[u], other)

    def swap_d(l, core, which):
        there = od.at[l, x, y, z, core, :, half(which, HD)]
        return remote(wd.at[l, :, half(theirs, HD)], there, csend.at[PAIR * L + l], crecv.at[PAIR * L + l], other)

    for u in range(PAIR * L):
        swap_g(u).start()
    for l in BOTH:
        swap_d(l, c, theirs).start()
        od[l, x, y, z, c, :, half(mine, HD)] = wd[l, :, half(mine, HD)]

    def zcopy(s, k):
        back = k % 2
        cols = GATE.part(s, back, s * GATE.width) if k >= 2 else pl.ds(s * GATE.width, GATE.width)
        v = zb.at[here.at[Z][0 if k < 2 else (2 * back - 1) % RING], :, cols]
        return remote(v, v, zsend.at[s, k], zrecv.at[s, k], here.moved(Z, 1 - 2 * back))

    for u in range(PAIR * L):
        swap_g(u).wait_recv()
        own, got = up(wg[u, :, half(mine, HG)]), up(cx[u])
        for core in range(PAIR):
            row = (u * PAIR + core) * ROWS
            cs[row : row + ROWS] = jnp.where(c == core, own, got)[0:ROWS]
    for s in BOTH:
        cols = slice(s * GATE.width, (s + 1) * GATE.width)
        zb[z, :, cols] = cs[:, cols].astype(BF)
        for k in BOTH:
            zcopy(s, k).start()
    gate = [Gathered(here, GATE, (o0, o1), (gsend, grecv), u, s) for u in range(PAIR * L) for s in BOTH]
    down = [Gathered(here, DOWN, (od,), (dsend, drecv), l, s) for l in BOTH for s in BOTH]
    for l in BOTH:
        swap_d(l, 1 - c, mine).wait_recv()
    for st in down:
        st.start(0)
    for s in BOTH:
        for k in BOTH:
            zcopy(s, k).wait_recv()
            zcopy(s, 2 + k).start()
    for st in down:
        st.forward(0)

    for s in BOTH:
        cols = slice(s * GATE.width, (s + 1) * GATE.width)
        for k in range(2, 4):
            zcopy(s, k).wait_recv()
        for i in range(RING):
            zm[...] = up(zb[i, :, cols])
            for u in range(PAIR * L):
                n = PAIR * ROWS
                zf[u, i * n : i * n + n] = zm[u * n : u * n + n]
        for st in gate[s::2]:
            (o0, o1)[st.u // L][st.u % L, x, y, 0, :, st.whole[0]] = zf[st.u].astype(BF)
            st.start(1)
    for st in down:
        st.end(0)
    both = gate[: L * 2] + down[:2] + gate[L * 2 :] + down[2:]
    for phase in (1, 2):
        for st in both:
            st.forward(phase)
        for st in both:
            st.end(phase)
    for u in range(PAIR * L):
        swap_g(u).wait_send()
    for l in BOTH:
        swap_d(l, c, theirs).wait_send()
    for s in BOTH:
        for k in range(4):
            zcopy(s, k).wait_send()
    for st in both:
        for phase in range(1 if st.cut.gate else 0, PHASES):
            for k in range(4):
                st.copy(phase, k).wait_send()
        for r in range(RING):
            st.across(r).wait_send()
            st.across(r, 1).wait_recv()


def ag(wg, wd):
    block = (RING, RING, 1, ZROWS, FF)
    outs = [pltpu.VMEM((L,) + block, BF)] * 2 + [pltpu.VMEM((L, RING, RING, RING, PAIR, DROWS, D), BF)]
    n, sems = PAIR * L, PHASES * 4 + RING
    scratch = [vmem((ZROWS, HG), F32), vmem((n, 16, HG), BF), vmem((RING, ZROWS, HG), BF), vmem((n, ZROWS, GATE.width), F32), vmem((ZROWS, GATE.width), F32)]
    scratch += [dma((n + L,))] * 2 + [dma((2, 4))] * 2 + [dma((n, 2, sems))] * 2 + [dma((L, 2, sems))] * 2
    return call(ag_kernel, outs, [VM] * 2, scratch, "ag", vmem_limit=5 * 2**20, ident=3, out_specs=[VM] * 3)(wg, wd)


def put_kernel(src, dst, sem):
    copies = [pltpu.make_async_copy(src.at[l, x], dst.at[l, x], sem.at[l, x]) for l in BOTH for x in range(RING)]
    for cp in copies:
        cp.start()
    for cp in copies:
        cp.wait()


def put(w):
    return call(put_kernel, [out(w.shape, BF)], [VM], [dma((L, RING))], "put", vmem_limit=2**20)(w)[0]


def device_step(x, dy, wg, wu, wd, *moments):
    x, dy = x[0], dy[0]
    a0, hid0, by_gate, by_up, h1, a1, hid1, d1 = forward(x, dy, wg, wu, wd)
    d0, pd0, gg1, gd1, squares1 = back(d1, h1, dy, wg, wu, wd, by_gate, by_up, hid0, *dw(a1, d1, hid1, dy))
    gg0, gd0, norm = end(a0, d0, pd0, squares1)
    moments, ng, nd = adamw((gg0, gg1, gd0, gd1), norm, moments, (wg, wu, wd))
    return (*(put(new).reshape(w.shape) for new, w in zip(ag(ng, nd), (wg, wu, wd))), *moments)


def solution(mesh):
    rows, moment, whole = P(("rep", "dp"), None, None), P(None, "dp", None), P(None, None, None)
    return jax.shard_map(
        device_step,
        mesh=mesh,
        in_specs=(rows,) * 2 + (whole,) * 3 + (moment,) * 6,
        out_specs=(P("rep", None, None),) * 3 + (P("rep", "dp", None),) * 6,
        check_vma=False,
    )
```

```python
import functools

import jax
import jax.numpy as jnp
from jax import lax
from jax.experimental import pallas as pl
from jax.experimental.pallas import tpu as pltpu
from jax.sharding import PartitionSpec as P

BF, F32 = jnp.bfloat16, jnp.float32
T, D, FF = 1024, 1280, 3072
L, RING, PAIR = 2, 4, 2
X, Y, Z, CORE = range(4)
HG, HD = FF // PAIR, D // PAIR
ROWS, DROWS = D // (RING**3 * PAIR), FF // (RING**3 * PAIR)
ZROWS = PAIR * RING * ROWS
NT = 256
WIDE = 512
PAD = 24
MOST = 67043328
HBM, VM = pl.BlockSpec(memory_space=pltpu.HBM), pl.BlockSpec(memory_space=pltpu.VMEM)
dma, vmem = pltpu.SemaphoreType.DMA, pltpu.VMEM
out = jax.ShapeDtypeStruct
ALL, BOTH = slice(None), range(2)
PAIR_SEM, PAIRS_SEM = dma((2,)), dma((2, 2))


class Place:
    def __init__(self):
        i = lax.axis_index("dp")
        chip, core = lax.div(i, PAIR), lax.rem(i, PAIR)
        self.at = [[lax.div(chip, RING**2)], [lax.rem(lax.div(chip, RING), RING)], [lax.rem(chip, RING)], [core, 1 - core]]
        for steps in self.at[:CORE]:
            steps += [lax.rem(steps[0] + r, RING) for r in range(1, RING)]
        self.peers = {}

    def moved(self, dim, by=1):
        by %= len(self.at[dim])
        if (dim, by) not in self.peers:
            x, y, z, core = (steps[by if d == dim else 0] for d, steps in enumerate(self.at))
            self.peers[dim, by] = {"dp": ((x * RING + y) * RING + z) * PAIR + core}
        return self.peers[dim, by]


def meet(peers):
    barrier = pltpu.get_barrier_semaphore()
    for peer in peers:
        pl.semaphore_signal(barrier, inc=1, device_id=peer)
    pl.semaphore_wait(barrier, len(peers))


def remote(src, dst, send, recv, peer):
    return pltpu.make_async_remote_copy(src, dst, send, recv, device_id=peer)


def up(v):
    return v.astype(F32)


def call(kernel, outs, ins, scratch, name, vmem_limit=MOST, ident=None, out_specs=None, **more):
    return pl.pallas_call(
        kernel,
        out_shape=outs,
        in_specs=ins,
        out_specs=out_specs or [HBM] * len(outs),
        scratch_shapes=scratch,
        compiler_params=pltpu.CompilerParams(collective_id=ident, has_side_effects=ident is not None, vmem_limit_bytes=vmem_limit),
        name=name,
        **more,
    )


def odd(i):
    return lax.rem(i, 2)


def tiled(n, body, hooks=(), base=0):
    def one(i, _):
        body(i)
        for k, hook in hooks:
            pl.when(base + i == k)(hook)
        return _

    lax.fori_loop(0, n, one, 0)


class Loaded:
    def __init__(self, n, src, buf, sem):
        self.n, self.src, self.buf, self.sem = n, src, buf, sem

    def copy(self, i):
        slot = odd(i)
        return pltpu.make_async_copy(self.src(i), self.buf.at[slot], self.sem.at[slot])

    def start(self):
        self.copy(jnp.int32(0)).start()

    def ready(self, i):
        pl.when(i + 1 < self.n)(lambda: self.copy(i + 1).start())
        self.copy(i).wait()

    def take(self, i):
        self.ready(i)
        return odd(i)


def mm(a, b, across=0):
    return lax.dot_general(a, b, (((1,), (across,)), ((), ())), preferred_element_type=F32)


def tn(a, b):
    return lax.dot_general(a, b, (((0,), (0,)), ((), ())), preferred_element_type=F32).astype(BF)


def at(i, n, base=0):
    return pl.ds(pl.multiple_of(base + i * n, 128), n)


def fetch(pairs, sem):
    copies = [pltpu.make_async_copy(src, dst, sem.at[i]) for i, (src, dst) in enumerate(pairs)]
    for cp in copies:
        cp.start()
    return copies


class Cut:
    def __init__(self, gate):
        self.gate = gate
        self.width = HG // 2 if gate else HD
        self.n, self.rows = (1, ZROWS) if gate else (RING, DROWS)

    def dims(self, s):
        return (s, 1 - s, Z) if self.gate else (Z, s, 1 - s)

    def part(self, s, h, base=0):
        first = 384 if self.gate or s == 0 else 256
        return pl.ds(base + first, self.width - first) if h else pl.ds(base, first)

    def index(self, here, s, dim, r, done, cols):
        at = [here.at[d][r % RING] if d == dim else ALL if d in done else here.at[d][0] for d in (X, Y, Z)]
        return (at[X], at[Y]) + ((ALL,) if self.gate else (at[Z], s)) + (ALL, cols)


GATE, DOWN = Cut(True), Cut(False)


def ahead(k):
    return 1 if k in (0, 3, 4) else -1


SUM, OWN, GOT = range(3)
TILES = 6
TILE = FF // TILES
DOWN_SCRATCH = [vmem((TILES, TILE, HD), BF)] + [dma((TILES,))] * 2 + [dma((GOT + 1, TILES))]
HIDDEN = [vmem((2, T, TILE), BF), PAIR_SEM, vmem((TILES, PAIR, TILE, HD), BF)]
BLOCKS = (RING, RING, 1, ZROWS)
GATE_SCRATCH = [vmem((2, 2) + BLOCKS + (GATE.width,), BF)] * 3 + [PAIRS_SEM] * 2
GATE_SUMS, DOWN_SUMS = out((GOT + 1, 2) + BLOCKS + (HG,), BF), out((GOT + 1, FF, HD), BF)


class DownProduct:
    def __init__(self, here, hid, hbuf, hsem, halves, got, send, recv, outsem):
        self.here, self.halves, self.got, self.send, self.recv, self.outsem = here, halves, got, send, recv, outsem
        self.hidden = Loaded(TILES, lambda i: hid.at[:, at(i, TILE)], hbuf, hsem)
        self.hidden.start()

    def swap(self, i):
        _, theirs = self.here.at[CORE]
        return remote(self.halves.at[i, theirs], self.got.at[i], self.send.at[i], self.recv.at[i], self.here.moved(CORE))

    def put(self, od, i):
        mine, theirs = self.here.at[CORE]
        srcs = self.halves.at[i, theirs], self.halves.at[i, mine], self.got.at[i]
        return [pltpu.make_async_copy(src, od.at[k, at(i, TILE), :], self.outsem.at[k, i]) for k, src in enumerate(srcs)]

    def run(self, dy, od, hooks=()):
        mine, theirs = self.here.at[CORE]

        def add(i):
            self.swap(i).wait()
            self.halves[i, theirs] = (up(self.got[i]) + up(self.halves[i, mine])).astype(BF)
            for cp in self.put(od, i):
                cp.start()

        def body(i):
            full = tn(self.hidden.buf[self.hidden.take(i)], dy[...])
            for half in BOTH:
                self.halves[i, half] = full[:, half * HD : (half + 1) * HD]
            self.swap(i).start()
            pl.when(i > 0)(lambda: add(i - 1))

        tiled(TILES, body, hooks)
        add(TILES - 1)
        for i in range(TILES):
            for cp in self.put(od, i):
                cp.wait()


class GateProducts:
    def __init__(self, here, d, buf, sem, total, own, got, send, recv):
        self.here, self.sems = here, (send, recv)
        self.terms = total, own, got

        def src(i):
            t, (mine, theirs) = lax.rem(i, 4), here.at[CORE]
            return d.at[lax.div(i, 4), :, at(odd(i), GATE.width, jnp.where(t < 2, theirs, mine) * HG)]

        self.tiles = Loaded(8, src, buf, sem)
        self.tiles.start()

    def swap(self, w, t):
        send, recv = self.sems
        return remote(self.terms[SUM].at[w, t], self.terms[GOT].at[w, t], send.at[w, t], recv.at[w, t], self.here.moved(CORE))

    def put(self, og, sem, w, t):
        return [pltpu.make_async_copy(v.at[w, t], og.at[k, w, :, :, :, :, at(t, GATE.width)], sem.at[k, w, t]) for k, v in enumerate(self.terms)]

    def run(self, a, hooks=(), after=lambda w, t: None):
        total, own, got = self.terms

        def product(i):
            return tn(a[...], self.tiles.buf[self.tiles.take(i)]).reshape(BLOCKS + (GATE.width,))

        def matrix(w, _):
            def theirs(t):
                total[w, t] = product(4 * w + t)
                self.swap(w, t).start()

            def mine(t):
                own[w, t] = product(4 * w + 2 + t)
                self.swap(w, t).wait()
                total[w, t] = (up(got[w, t]) + up(own[w, t])).astype(BF)
                after(w, t)

            tiled(2, theirs, hooks, 4 * w)
            tiled(2, mine, hooks, 4 * w + 2)
            return _

        lax.fori_loop(0, 2, matrix, 0)


COLUMNS = [vmem((2, T, GATE.width), BF), PAIR_SEM]


PART = T // 4


def in_parts(body, at_once=T // PART):
    def some(i):
        for k in range(at_once):
            body(at(at_once * i + k, PART))

    tiled(T // (at_once * PART), some)


def normed(src, dst):
    def rows(i):
        r = at(i, PART)
        wide = up(src[r])
        dst[r] = (wide * lax.rsqrt(jnp.mean(wide**2, -1, keepdims=True) + 1e-6)).astype(BF)

    tiled(T // PART, rows)


def gated(gate, u):
    sig = jax.nn.sigmoid(gate)
    silu = gate * sig
    return (silu * u).astype(BF), u * (sig * (1 + gate * (1 - sig))), silu


class Stored:
    def __init__(self, dst, buf, sem):
        self.dst, self.buf, self.sem = dst, buf, sem

    def copy(self, i):
        slot = odd(i)
        return pltpu.make_async_copy(self.buf.at[slot], self.dst(i), self.sem.at[slot])

    def free(self, i):
        pl.when(i >= 2)(lambda: self.copy(i - 2).wait())

    def end(self, n):
        for i in (n - 2, n - 1):
            self.copy(jnp.int32(i)).wait()


HALVES = vmem((2, 2, D, WIDE), BF)
STATES = vmem((T, D), BF)


def forward_kernel(x, dy, wg, wu, wd, oa0, ohid0, ofg, ofu, oh1, ohid1, od1, og, od, vx, va, vhid, vdy, sem, osem, hsem, *refs):
    n, here = FF // WIDE, Place()
    meet([here.moved(CORE)])
    x_here, dy_here = fetch([(x, vx), (dy, vdy)], sem)
    wide = lambda ref, l: lambda i: ref.at[l, :, at(i, WIDE)]

    def put(i):
        return pltpu.make_async_copy(vhid.at[:, at(i, WIDE)], ohid0.at[:, at(i, WIDE)], hsem.at[i])

    def first(vw, wsem, vo, vsem):
        tiles = [Loaded(n, wide(w, 0), vw.at[k], wsem.at[k]) for k, w in enumerate((wg, wu))]
        outs = [Stored(lambda i, o=o: o.at[:, at(i, WIDE)], vo.at[k], vsem.at[k]) for k, o in enumerate((ofg, ofu))]
        for t in tiles:
            t.start()
        x_here.wait()
        normed(vx, va)
        a_out, = fetch([(va, oa0)], osem)

        def body(i):
            slot, _ = [t.take(i) for t in tiles]
            for o in outs:
                o.free(i)

            def rows(r):
                vhid[r, at(i, WIDE)], *factors = gated(*(mm(va[r], vw[k, slot]) for k in BOTH))
                for k in BOTH:
                    vo[k, slot, r] = factors[k]

            in_parts(rows)
            put(i).start()
            for o in outs:
                o.copy(i).start()

        tiled(n, body)
        for o in outs:
            o.end(n)
        a_out.wait()

    pl.run_scoped(first, HALVES, PAIRS_SEM, vmem((2, 2, T, WIDE), F32), PAIRS_SEM)

    def second(vw, wsem):
        tiles = Loaded(D // NT, lambda i: wd.at[0, :, at(i, NT)], vw, wsem)
        tiles.start()

        def body(i):
            slot, cols = tiles.take(i), at(i, NT)

            def rows(r):
                vx[r, cols] = (up(vx[r, cols]) + up(mm(vhid[r], vw[slot]).astype(BF))).astype(BF)

            in_parts(rows)

        tiled(D // NT, body)

    pl.run_scoped(second, vmem((2, FF, NT), BF), PAIR_SEM)
    for i in range(n):
        put(i).wait()

    def third(vw, wsem, vd, dsem, vo, vsem):
        tiles = [Loaded(n, wide(w, 1), vw.at[k], wsem.at[k]) for k, w in enumerate((wg, wu))]
        tiles.append(Loaded(n, lambda i: wd.at[1, at(i, WIDE), :], vd, dsem))
        outs = [Stored(lambda i, o=o: o.at[:, at(i, WIDE)], vo.at[k], vsem.at[k]) for k, o in enumerate((od1.at[0], od1.at[1], ohid1))]
        for t in tiles:
            t.start()
        normed(vx, va)
        kept = fetch([(vx, oh1)], osem)
        dy_here.wait()

        def body(i):
            slot, *_ = [t.take(i) for t in tiles]
            for o in outs:
                o.free(i)

            def rows(r):
                hid, *factors = gated(*(mm(va[r], vw[k, slot]) for k in BOTH))
                dhid = up(mm(vdy[r], vd[slot], 1).astype(BF))
                vo[2, slot, r] = hid
                for k in BOTH:
                    vo[k, slot, r] = (dhid * factors[k]).astype(BF)

            in_parts(rows)
            for o in outs:
                o.copy(i).start()

        tiled(n, body)
        for o in outs:
            o.end(n)
        for cp in kept:
            cp.wait()

    pl.run_scoped(third, HALVES, PAIRS_SEM, vmem((2, WIDE, D), BF), PAIR_SEM, vmem((3, 2, T, WIDE), BF), dma((3, 2)))

    def fourth(*local):
        k = len(HIDDEN)
        down = DownProduct(here, ohid1, *local[:k], *refs[: len(DOWN_SCRATCH)])
        *gate_refs, gsem = refs[len(DOWN_SCRATCH) :]
        gates = GateProducts(here, od1, *local[k:], *gate_refs)

        def put(w, t):
            for cp in gates.put(og, gsem, w, t):
                cp.start()

        down.run(vdy, od)
        gates.run(va, after=put)
        for w in BOTH:
            for t in BOTH:
                for cp in gates.put(og, gsem, w, t):
                    cp.wait()

    pl.run_scoped(fourth, *HIDDEN, *COLUMNS, *GATE_SCRATCH[:GOT])


def forward(x, dy, wg, wu, wd):
    states, hidden = out((T, D), BF), out((T, FF), BF)
    outs = [states, hidden, out((T, FF), F32), out((T, FF), F32), states, hidden, out((2, T, FF), BF), GATE_SUMS, DOWN_SUMS]
    scratch = [STATES] * 2 + [vmem((T, FF), BF), STATES, PAIR_SEM, PAIR_SEM, dma((FF // WIDE,))]
    scratch += DOWN_SCRATCH + GATE_SCRATCH[GOT:] + [dma((GOT + 1, 2, 2))]
    a0, hid0, by_gate, by_up, h1, _, d1, pg, pd = call(forward_kernel, outs, [HBM] * 5, scratch, "forward", ident=1)(x, dy, wg, wu, wd)
    return a0, hid0, by_gate, by_up, h1, d1, pg, pd


PHASES, COPIES = 3, 6
NAMES = ("r1", "o1", "k2", "r2", "t3", "k3", "r3", "send", "recv", "own")


class Summed:
    def __init__(self, here, cut, src, b, u, s):
        self.here, self.cut, self.src, self.us, self.s, self.dims = here, cut, src, (u, s), s, cut.dims(s)
        self.got, self.kept = [b[k] for k in ("r1", "r2", "r3")], [b[k] for k in ("o1", "k2", "k3")]
        self.t3, self.sems, self.direct = b["t3"], (b["send"], b["recv"], b["own"]), isinstance(src, tuple)

    def block(self, phase, r, cols=ALL, first=()):
        dim = self.dims[phase]
        i = self.here.at[dim][r % RING]
        if phase == 2:
            return self.us + first + (i, ALL, cols)
        second = phase == 1 and not self.cut.gate and self.s
        return self.us + first + ((ALL, i) if second else (i, ALL)) + (ALL, cols)

    def first(self, kind, r, h):
        if self.direct:
            ref, lead, base = self.src[kind], self.us, 0
        else:
            ref, lead, base = self.src, (kind,) + (self.us[:1] if self.cut.gate else ()), self.s * self.cut.width if self.cut.gate else 0
        return ref.at[lead + self.cut.index(self.here, self.s, self.dims[0], r, self.dims, self.cut.part(self.s, h, base))]

    def term(self, n, cols=ALL, r=0):
        if self.direct:
            i = self.here.at[self.dims[0]][r % RING]
            at_, terms = [self.us + ((n, i) if self.s else (i, n)) + (ALL, ALL, cols)] * 2, self.src[OWN:]
        else:
            at_, terms = [self.us + (k, n, ALL, ALL, cols) for k in BOTH], [self.kept[0]] * 2
        return sum(up(ref[i]) for ref, i in zip(terms, at_))

    def at(self, phase, kind, cols=ALL):
        return self.us + (kind,) + (ALL,) * (PHASES - phase) + (cols,)

    def copy(self, phase, k):
        kind, h = k // 2, k % 2
        cols = self.cut.part(self.s, h)
        got = self.got[phase]
        r = (2, -ahead(h), 0)[kind]
        if kind == 2:
            src = got.at[self.at(phase, 0, cols)]
        elif phase == 0:
            src = self.first(SUM, r, h)
        elif phase == 1:
            src = self.got[0].at[self.block(1, r, cols, (2,))]
        else:
            src = self.t3.at[self.block(2, r, cols)]
        send, recv, _ = self.sems
        i = self.us + (phase * COPIES + k,)
        return remote(src, got.at[self.at(phase, kind, cols)], send.at[i], recv.at[i], self.here.moved(self.dims[phase], ahead(k)))

    def own(self, k):
        kind, h = k // 2, k % 2
        cols, copies = self.cut.part(self.s, h), []
        for term in () if self.direct else BOTH:
            dst = self.kept[0].at[self.us + (term,) + (ALL,) * PHASES + (cols,)]
            copies.append(pltpu.make_async_copy(self.first(OWN + term, 0 if kind else ahead(h), h), dst, self.sems[2].at[self.us + (k, term)]))
        return copies

    def start(self, part):
        for h in BOTH:
            self.copy(0, 2 * part + h).start()
            for cp in [] if part else self.own(h):
                cp.start()

    def arrive(self, ks):
        for k in ks:
            for cp in self.own(k):
                cp.wait()

    def pass_on(self, phase):
        got, kept = self.got[phase], self.kept[phase]
        for h in BOTH:
            self.copy(phase, h).wait_recv()
            cols = self.cut.part(self.s, h)
            if phase:
                i = self.at(phase, 0, cols)
                got[i] = (up(got[i]) + kept[self.block(phase, ahead(h), cols)]).astype(BF)
            else:
                self.arrive([h])

                def add(n):
                    i = self.us + (0, n, ALL, ALL, cols)
                    got[i] = (up(got[i]) + self.term(n, cols, ahead(h))).astype(BF)

                tiled(RING, add)
            self.copy(phase, 4 + h).start()
        for h in () if phase else BOTH:
            for cp in self.own(2 + h):
                cp.start()

    def finish(self, phase):
        for k in range(2, COPIES):
            self.copy(phase, k).wait_recv()
        got, kept = self.got[phase], self.kept[phase]
        if phase:
            return kept[self.block(phase, 0)] + up(got[self.us + (2,)]) + up(got[self.us + (1,)])
        self.arrive((2, 3))

        def add(n):
            total = self.term(n) + up(got[self.us + (2, n)]) + up(got[self.us + (1, n)])
            self.kept[1][self.us + (n,)] = total
            got[self.us + (2, n)] = total.astype(BF)

        tiled(RING, add)

    def starts(self, phase):
        for k in range(4):
            self.copy(phase, k).start()


class Sums:
    def __init__(self, here, og, od, refs):
        self.here = here
        n = len(NAMES)
        bufs = [dict(zip(NAMES, refs[i : i + n])) for i in (0, n)]
        self.f3, self.f4, self.ce, self.cr, self.co, self.fd, self.dr, self.csend, self.crecv, self.putsem = refs[2 * n :]
        self.gate, self.upper = ([Summed(here, GATE, og, bufs[0], u, s) for s in BOTH] for u in BOTH)
        self.down = [Summed(here, DOWN, od, bufs[1], 0, s) for s in BOTH]
        self.puts = []
        self.f3[ZROWS : ZROWS + 8] = jnp.zeros((8, GATE.width), F32)
        self.f4[PAD : PAD + 8] = jnp.zeros((8, HG), F32)

    def begin(self, streams):
        for part in BOTH:
            for st in streams:
                st.start(part)

    def second(self, st):
        total = st.finish(1)
        if st.cut.gate:
            self.f3[0:ZROWS] = total[0]
            for i in range(RING):
                rows = self.f3[i * PAIR * ROWS : i * PAIR * ROWS + PAD]
                st.kept[2][st.us + (i,)] = rows
                st.t3[st.us + (i,)] = rows.astype(BF)
        else:
            st.kept[2][st.us] = total
            st.t3[st.us] = total.astype(BF)

    def step(self, n, *streams):
        for st in streams:
            if n % 2 == 0:
                st.pass_on(n // 2)
            else:
                if n == 1:
                    st.finish(0)
                else:
                    self.second(st)
                st.starts(n // 2 + 1)

    def swap(self, u):
        src, dst = (self.fd.at[self.here.at[CORE][1]], self.dr) if u == 2 else (self.ce.at[u], self.cr.at[u])
        return remote(src, dst, self.csend.at[u], self.crecv.at[u], self.here.moved(CORE))

    def last(self, u):
        if u == 2:
            for st in self.down:
                self.fd[st.s] = st.finish(2).astype(BF)
            parts = [up(self.fd[s]) for s in BOTH]
        else:
            for st in self.upper if u else self.gate:
                self.f4[0:PAD, st.s * GATE.width : (st.s + 1) * GATE.width] = st.finish(2)
            low, high = self.f4[0:16], self.f4[ROWS : ROWS + 16]
            first = self.here.at[CORE][0] == 0
            self.co[u] = jnp.where(first, low, high).astype(BF)
            self.ce[u] = jnp.where(first, high, low).astype(BF)
            valid = lax.broadcasted_iota(jnp.int32, (PAD, HG), 0) < PAIR * ROWS
            parts = [jnp.where(valid, up(self.f4[0:PAD].astype(BF)), 0.0)]
        self.swap(u).start()
        return sum(squares(v) for v in parts)

    def put(self, src, dst):
        self.puts.append(pltpu.make_async_copy(src, dst, self.putsem.at[len(self.puts)]))
        self.puts[-1].start()

    def results(self, gg, gd):
        mine, theirs = self.here.at[CORE]
        for u in range(3):
            n, dst = (HD, gd) if u == 2 else (HG, gg.at[u])
            self.put(self.fd.at[mine] if u == 2 else self.co.at[u], dst.at[:, at(mine, n)])
            self.swap(u).wait()
            self.put(self.dr if u == 2 else self.cr.at[u], dst.at[:, at(theirs, n)])

    def drain(self):
        for st in self.down + self.gate + self.upper:
            for k in range(PHASES * COPIES):
                st.copy(k // COPIES, k % COPIES).wait_send()
        for cp in self.puts:
            cp.wait()


def squares(v):
    v = v * v
    rows = sum(v[i : i + 8] for i in range(0, v.shape[0], 8))
    return sum(rows[:, i : i + 128] for i in range(0, v.shape[1], 128))


LANES = vmem((8, 128), F32)


def sums_scratch(direct):
    scratch = []
    for cut, units in ((GATE, 2), (DOWN, 1)):
        us, block, width = (units, 2), (cut.n, cut.rows, cut.width), cut.width
        terms = LANES if direct and cut.gate else vmem(us + (2, RING) + block, BF)
        scratch += [vmem(us + (3, RING) + block, BF), terms, vmem(us + (RING,) + block, F32), vmem(us + (3,) + block, BF)]
        scratch += [vmem(us + (RING, PAD, width), t) for t in (BF, F32)] + [vmem(us + (3, PAD, width), BF)]
        scratch += [dma(us + (PHASES * COPIES,))] * 2 + [dma(us + (4, 2))]
    scratch += [vmem((ZROWS + 8, GATE.width), F32), vmem((PAD + 8, HG), F32)] + [vmem((2, 16, HG), BF)] * 3
    return scratch + [vmem((2, DROWS, HD), BF), vmem((DROWS, HD), BF)] + [dma((3,))] * 2 + [dma((7,))]


ROWS_OUT = [out((2, 16, FF), BF), out((DROWS, D), BF), out((8, 128), F32)]
DOWN_BLOCKS = (GOT + 1, RING, RING, RING, PAIR, DROWS, HD)


def all_peers(here):
    return [here.moved(d, r) for d in (X, Y, Z) for r in range(1, RING)] + [here.moved(CORE)]


def over_all(here, total, nb, nr, send, recv):
    n = 0
    for stage, dim in enumerate((CORE, Z, Y, X)):
        nb[stage] = total
        copies = []
        for r in range(1, len(here.at[dim])):
            copies.append(remote(nb.at[stage], nr.at[n], send.at[n], recv.at[n], here.moved(dim, r)))
            copies[-1].start()
            n += 1
        for i, cp in enumerate(copies):
            cp.wait()
            total = total + nr[n - len(copies) + i]
    return total


def back_kernel(d, h1, dy, wg, wu, wd, by_gate, by_up, hid, pg, pd, od0, opd, gg, gd, osq, dx, vh, vy, nb, sem, state_sem, *refs):
    here = Place()
    n = len(DOWN_SCRATCH)
    sums = Sums(here, pg, pd, refs[n:])
    meet(all_peers(here))
    step = lambda n, streams: lambda: sums.step(n, *streams)
    early, late = zip(sums.down, sums.gate[:1] + sums.upper[:1], sums.gate[1:] + sums.upper[1:])
    sums.begin(early + late)
    states_here = fetch([(h1, vh), (dy, vy)], state_sem)

    def states(vd, vw, wsem):
        n = D // NT
        tiles = [Loaded(n, lambda i, w=w: w.at[1, at(i, NT), :], vw.at[k], wsem.at[k]) for k, w in enumerate((wg, wu))]
        loads = []
        for k in BOTH:
            loads += fetch([(d.at[k], vd.at[k])], sem.at[pl.ds(k, 1)])
            tiles[k].start()

        def body(i):
            k, i = lax.div(i, n), lax.rem(i, n)
            for which in BOTH:
                pl.when(k == which)(lambda: tiles[which].ready(i))
            before = jnp.where(k == 0, 0.0, up(dx[:, at(i, NT)]))
            dx[:, at(i, NT)] = (before + up(mm(vd[k], vw[k, odd(i)], 1).astype(BF))).astype(BF)

        hooks = [(n - 1, loads[1].wait), (n // 2, step(0, early)), (n + 1, step(0, late))]
        loads[0].wait()
        tiled(2 * n, body, hooks)

    pl.run_scoped(states, vmem((2, T, FF), BF), vmem((2, 2, NT, FF), BF), PAIRS_SEM)

    def norm_back(i):
        r = at(i, NT)
        wide, da = up(vh[r]), up(dx[r])
        scale = lax.rsqrt(jnp.mean(wide**2, -1, keepdims=True) + 1e-6)
        mean = jnp.mean(da * wide, -1, keepdims=True)
        dx[r] = (up(vy[r]) + up((da * scale - wide * (scale * scale * scale * mean)).astype(BF))).astype(BF)

    for cp in states_here:
        cp.wait()
    tiled(T // NT, norm_back)

    def hidden_back(vw, wsem, vf, fsem, vo, outsem):
        n = FF // WIDE
        tiles = [Loaded(n, lambda i: wd.at[0, at(i, WIDE), :], vw, wsem)]
        tiles += [Loaded(n, lambda i, f=f: f.at[:, at(i, WIDE)], vf.at[k], fsem.at[k]) for k, f in enumerate((by_gate, by_up))]
        outs = [Stored(lambda i, k=k: od0.at[k, :, at(i, WIDE)], vo.at[k], outsem.at[k]) for k in BOTH]
        for t in tiles:
            t.start()

        def body(i):
            slot, *_ = [t.take(i) for t in tiles]
            for o in outs:
                o.free(i)

            def rows(r):
                dhid = up(mm(dx[r], vw[slot], 1).astype(BF))
                for k in BOTH:
                    vo[k, slot, r] = (dhid * vf[k, slot, r]).astype(BF)

            in_parts(rows, 2)
            for o in outs:
                o.copy(i).start()

        tiled(n, body, [(1, step(1, early)), (3, step(1, late)), (4, step(2, early)), (5, step(2, late))])
        for o in outs:
            o.end(n)

    pl.run_scoped(hidden_back, vmem((2, WIDE, D), BF), PAIR_SEM, vmem((2, 2, T, WIDE), F32), PAIRS_SEM, vmem((2, 2, T, WIDE), BF), PAIRS_SEM)

    def last(*tile_refs):
        steps = [step(n, streams) for n in (3, 4) for streams in (early, late)]
        DownProduct(here, hid, *tile_refs, *refs[:n]).run(dx, opd, list(enumerate(steps)))

    pl.run_scoped(last, *HIDDEN)
    nb[...] = sum(sums.last(u) for u in (2, 0, 1))
    sums.results(gg, gd)
    sums.put(nb, osq)
    sums.drain()


def back(*args):
    *ins, pg, pd = args
    outs = [out((2, T, FF), BF), DOWN_SUMS] + ROWS_OUT
    scratch = [STATES] * 3 + [LANES, PAIR_SEM, PAIR_SEM] + DOWN_SCRATCH + sums_scratch(False)
    return call(back_kernel, outs, [HBM] * len(args), scratch, "back", ident=2)(*ins, pg, pd.reshape(DOWN_BLOCKS))


def end_kernel(a, d, pd, sq, gg, gd, osq, va, vsq, nb, nr, nsend, nrecv, sem, *refs):
    here = Place()
    n = len(COLUMNS + GATE_SCRATCH)
    gates = GateProducts(here, d, *refs[:n])
    sums = Sums(here, gates.terms, pd, refs[n:])
    a_here, sq_here = fetch([(a, va), (sq, vsq)], sem)
    meet(all_peers(here))
    sums.begin(sums.down)
    a_here.wait()
    (d0, d1), (g0, g1), (u0, u1) = sums.down, sums.gate, sums.upper

    def begin(new, *old):
        sums.begin([new])
        sums.step(0, *old)

    hooks = {2: lambda: begin(g0), 3: lambda: begin(g1, d0), 4: lambda: sums.step(0, d1), 5: lambda: sums.step(0, g0), 6: lambda: begin(u0, g1)}
    gates.run(va, hooks.items())
    sums.begin([u1])
    sums.step(1, g0, d0, g1)
    sums.step(0, u0)
    sums.step(1, d1)
    sums.step(0, u1)
    for n in (2, 3):
        sums.step(n, g0, d0, g1, d1)
    sums.step(1, u0, u1)
    sums.step(4, g0, d0, g1, d1)
    sums.step(2, u0, u1)
    total = sums.last(2) + sums.last(0)
    for n in (3, 4):
        sums.step(n, u0, u1)
    total += sums.last(1)
    sq_here.wait()
    nb[4] = over_all(here, total + vsq[...], nb, nr, nsend, nrecv)
    sums.put(nb.at[4], osq)
    sums.results(gg, gd)
    sums.drain()


def end(a, d, pd, sq):
    scratch = [STATES, LANES, vmem((5, 8, 128), F32), vmem((10, 8, 128), F32)] + [dma((10,))] * 2 + [PAIR_SEM]
    scratch += COLUMNS + GATE_SCRATCH + sums_scratch(True)
    return call(end_kernel, ROWS_OUT, [HBM] * 4, scratch, "end", ident=4)(a, d, pd.reshape(DOWN_BLOCKS), sq)


COUNT = 3 * L * D * FF


def adamw_kernel(gg0, gg1, gd0, gd1, norm, *refs):
    old, (wg, wu, wd), new, (ng, nd, win, wind, sg, sw, sem) = refs[:6], refs[6:9], refs[9:15], refs[15:]
    i = lax.axis_index("dp")
    start, off = pl.multiple_of(i * ROWS // 8 * 8, 8), i * ROWS % 8
    copies = [pltpu.make_async_copy((wg, wu)[u // L].at[u % L, pl.ds(start, 16), :], win.at[u], sem.at[u]) for u in range(PAIR * L)]
    copies.append(pltpu.make_async_copy(wd.at[:, pl.ds(pl.multiple_of(i * DROWS, 8), DROWS), :], wind, sem.at[PAIR * L]))
    for cp in copies:
        cp.start()
    factor = jnp.minimum(1.0, 0.5 * lax.rsqrt(jnp.full((1, 1), jnp.sum(norm[...])) / COUNT + 1e-30))
    for cp in copies:
        cp.wait()

    def step(k, w, g):
        g = g * factor
        m = 0.9 * old[k][...] + 0.1 * g
        v = 0.95 * old[k + 3][...] + 0.05 * g * g
        new[k][...], new[k + 3][...] = m, v
        return w - 0.02 * (m * lax.rsqrt(v + 1e-8) + 0.1 * w)

    for k in BOTH:
        for l in BOTH:
            w = up(win[k * L + l])
            rows = w[0:ROWS]
            for skip in (2, 4, 6):
                rows = jnp.where(off == skip, w[skip : skip + ROWS], rows)
            sw[:, l, :] = rows
            sg[:, l, :] = up((gg0, gg1)[l][k])[0:ROWS]
        sw[...] = step(k, sw[...], sg[...])
        for l in BOTH:
            ng[k * L + l, 0:ROWS] = sw[:, l, :].astype(BF)
    nd[...] = step(2, up(wind[...]), jnp.stack([up(gd0[...]), up(gd1[...])])).astype(BF)


def adamw(sums, norm, moments, weights):
    weights = [pltpu.with_memory_space_constraint(w, pltpu.HBM) for w in weights]
    flip = lambda k, t: t if k % 3 == 2 else jnp.swapaxes(t, 0, 1)
    moments = [flip(k, t) for k, t in enumerate(moments)]
    outs = [out(t.shape, F32) for t in moments] + [out((PAIR * L, 16, FF), BF), vmem((L, DROWS, D), BF)]
    scratch = [vmem((PAIR * L, 16, FF), BF), vmem((L, DROWS, D), BF)] + [vmem((ROWS, L, FF), F32)] * 2 + [dma((PAIR * L + 1,))]
    *new, ng, nd = call(adamw_kernel, outs, [VM] * 11 + [HBM] * 3, scratch, "adamw", MOST - 5 * 2**17, out_specs=[VM] * 8)(*sums, norm, *moments, *weights)
    return [flip(k, t) for k, t in enumerate(new)], ng, nd


class Gathered:
    def __init__(self, here, cut, refs, b, u, s):
        self.here, self.cut, self.refs, self.b, self.u, self.s = here, cut, refs, b, u, s
        self.order = cut.dims(s)[::-1]
        n, first = (HG, s * cut.width) if cut.gate else (HD, 0)
        self.whole = [pl.ds(pl.multiple_of(c * n + first, 128), cut.width) for c in here.at[CORE]]

    def ref(self, at):
        return self.refs[self.u // L].at[(self.u % L,) + at]

    def copy(self, phase, k):
        dim, back = self.order[phase], k % 2
        cols = self.whole[0]
        if k >= 2:
            cols = self.cut.part(self.s, back, cols.start)
        v = self.ref(self.cut.index(self.here, self.s, dim, 0 if k < 2 else 2 * back - 1, self.order[:phase], cols))
        i = phase * 4 + k
        return remote(v, v, self.b[0].at[self.u, self.s, i], self.b[1].at[self.u, self.s, i], self.here.moved(dim, 1 - 2 * back))

    def across(self, r, core=0):
        v = self.ref(self.cut.index(self.here, self.s, self.order[2], r, self.order, self.whole[core]))
        i = PHASES * 4 + r % RING
        return remote(v, v, self.b[0].at[self.u, self.s, i], self.b[1].at[self.u, self.s, i], self.here.moved(CORE))

    def start(self, phase):
        for k in BOTH:
            self.copy(phase, k).start()
        if phase == 2:
            self.across(0).start()

    def forward(self, phase):
        for k in BOTH:
            self.copy(phase, k).wait_recv()
            self.copy(phase, 2 + k).start()
            if phase == 2:
                self.across(2 * k - 1).start()

    def end(self, phase):
        for k in BOTH:
            self.copy(phase, 2 + k).wait_recv()
        if phase < 2:
            self.start(phase + 1)
        else:
            self.across(2).start()


def ag_kernel(wg, wd, o0, o1, od, cs, cx, zb, zf, zm, csend, crecv, zsend, zrecv, gsend, grecv, dsend, drecv):
    here = Place()
    (x, y, z, c), other = (steps[0] for steps in here.at), here.moved(CORE)
    meet([here.moved(d, r) for d in (X, Y, Z) for r in (1, -1)] + [other])
    half = lambda which, n: pl.ds(pl.multiple_of(which * n, 128), n)
    mine, theirs = c, 1 - c

    def swap_g(u):
        return remote(wg.at[u, :, half(theirs, HG)], cx.at[u], csend.at[u], crecv.at[u], other)

    def swap_d(l, core, which):
        there = od.at[l, x, y, z, core, :, half(which, HD)]
        return remote(wd.at[l, :, half(theirs, HD)], there, csend.at[PAIR * L + l], crecv.at[PAIR * L + l], other)

    for u in range(PAIR * L):
        swap_g(u).start()
    for l in BOTH:
        swap_d(l, c, theirs).start()
        od[l, x, y, z, c, :, half(mine, HD)] = wd[l, :, half(mine, HD)]

    def zcopy(s, k):
        back = k % 2
        cols = GATE.part(s, back, s * GATE.width) if k >= 2 else pl.ds(s * GATE.width, GATE.width)
        v = zb.at[here.at[Z][0 if k < 2 else (2 * back - 1) % RING], :, cols]
        return remote(v, v, zsend.at[s, k], zrecv.at[s, k], here.moved(Z, 1 - 2 * back))

    for u in range(PAIR * L):
        swap_g(u).wait_recv()
        own, got = up(wg[u, :, half(mine, HG)]), up(cx[u])
        for core in range(PAIR):
            row = (u * PAIR + core) * ROWS
            cs[row : row + ROWS] = jnp.where(c == core, own, got)[0:ROWS]
    for s in BOTH:
        cols = slice(s * GATE.width, (s + 1) * GATE.width)
        zb[z, :, cols] = cs[:, cols].astype(BF)
        for k in BOTH:
            zcopy(s, k).start()
    gate = [Gathered(here, GATE, (o0, o1), (gsend, grecv), u, s) for u in range(PAIR * L) for s in BOTH]
    down = [Gathered(here, DOWN, (od,), (dsend, drecv), l, s) for l in BOTH for s in BOTH]
    for l in BOTH:
        swap_d(l, 1 - c, mine).wait_recv()
    for st in down:
        st.start(0)
    for s in BOTH:
        for k in BOTH:
            zcopy(s, k).wait_recv()
            zcopy(s, 2 + k).start()
    for st in down:
        st.forward(0)

    for s in BOTH:
        cols = slice(s * GATE.width, (s + 1) * GATE.width)
        for k in range(2, 4):
            zcopy(s, k).wait_recv()
        for i in range(RING):
            zm[...] = up(zb[i, :, cols])
            for u in range(PAIR * L):
                n = PAIR * ROWS
                zf[u, i * n : i * n + n] = zm[u * n : u * n + n]
        for st in gate[s::2]:
            (o0, o1)[st.u // L][st.u % L, x, y, 0, :, st.whole[0]] = zf[st.u].astype(BF)
            st.start(1)
    for st in down:
        st.end(0)
    both = gate[: L * 2] + down[:2] + gate[L * 2 :] + down[2:]
    for phase in (1, 2):
        for st in both:
            st.forward(phase)
        for st in both:
            st.end(phase)
    for u in range(PAIR * L):
        swap_g(u).wait_send()
    for l in BOTH:
        swap_d(l, c, theirs).wait_send()
    for s in BOTH:
        for k in range(4):
            zcopy(s, k).wait_send()
    for st in both:
        for phase in range(1 if st.cut.gate else 0, PHASES):
            for k in range(4):
                st.copy(phase, k).wait_send()
        for r in range(RING):
            st.across(r).wait_send()
            st.across(r, 1).wait_recv()


def ag(wg, wd):
    block = (RING, RING, 1, ZROWS, FF)
    outs = [pltpu.VMEM((L,) + block, BF)] * 2 + [pltpu.VMEM((L, RING, RING, RING, PAIR, DROWS, D), BF)]
    n, sems = PAIR * L, PHASES * 4 + RING
    scratch = [vmem((ZROWS, HG), F32), vmem((n, 16, HG), BF), vmem((RING, ZROWS, HG), BF), vmem((n, ZROWS, GATE.width), F32), vmem((ZROWS, GATE.width), F32)]
    scratch += [dma((n + L,))] * 2 + [dma((2, 4))] * 2 + [dma((n, 2, sems))] * 2 + [dma((L, 2, sems))] * 2
    return call(ag_kernel, outs, [VM] * 2, scratch, "ag", vmem_limit=3 * 2**20, ident=3, out_specs=[VM] * 3)(wg, wd)


def put_kernel(*refs):
    *refs, sem = refs
    n = len(refs) // 2
    pairs = [(refs[k].at[l, x], refs[n + k].at[l, x]) for k in range(n) for l in BOTH for x in range(RING)]
    for cp in fetch(pairs, sem):
        cp.wait()


def put(weights):
    n = len(weights)
    return call(put_kernel, [out(w.shape, BF) for w in weights], [VM] * n, [dma((n * L * RING,))], "put", vmem_limit=2**20)(*weights)


def device_step(x, dy, wg, wu, wd, *moments):
    x, dy = x[0], dy[0]
    a0, hid0, by_gate, by_up, h1, d1, pg1, pd1 = forward(x, dy, wg, wu, wd)
    d0, pd0, gg1, gd1, squares1 = back(d1, h1, dy, wg, wu, wd, by_gate, by_up, hid0, pg1, pd1)
    gg0, gd0, norm = end(a0, d0, pd0, squares1)
    moments, ng, nd = adamw((gg0, gg1, gd0, gd1), norm, moments, (wg, wu, wd))
    return (*(new.reshape(w.shape) for new, w in zip(put(ag(ng, nd)), (wg, wu, wd))), *moments)


def solution(mesh):
    rows, moment, whole = P(("rep", "dp")), P(None, "dp"), P()
    return jax.shard_map(
        device_step,
        mesh=mesh,
        in_specs=(rows,) * 2 + (whole,) * 3 + (moment,) * 6,
        out_specs=(P("rep"),) * 3 + (P("rep", "dp"),) * 6,
        check_vma=False,
    )
```

```python
import functools

import jax
import jax.numpy as jnp
from jax import lax
from jax.experimental import pallas as pl
from jax.experimental.pallas import tpu as pltpu
from jax.sharding import PartitionSpec as P

BF, F32 = jnp.bfloat16, jnp.float32
T, D, FF = 1024, 1280, 3072
L, RING, PAIR = 2, 4, 2
X, Y, Z, CORE = range(4)
HG, HD = FF // PAIR, D // PAIR
ROWS, DROWS = D // (RING**3 * PAIR), FF // (RING**3 * PAIR)
ZROWS = PAIR * RING * ROWS
NT = 256
WIDE = 512
PAD = 24
MOST = 67043328
HBM, VM = pl.BlockSpec(memory_space=pltpu.HBM), pl.BlockSpec(memory_space=pltpu.VMEM)
dma, vmem = pltpu.SemaphoreType.DMA, pltpu.VMEM
out = jax.ShapeDtypeStruct
ALL, BOTH = slice(None), range(2)
PAIR_SEM, PAIRS_SEM = dma((2,)), dma((2, 2))


class Place:
    def __init__(self):
        i = lax.axis_index("dp")
        chip, core = lax.div(i, PAIR), lax.rem(i, PAIR)
        self.at = [[lax.div(chip, RING**2)], [lax.rem(lax.div(chip, RING), RING)], [lax.rem(chip, RING)], [core, 1 - core]]
        for steps in self.at[:CORE]:
            steps += [lax.rem(steps[0] + r, RING) for r in range(1, RING)]
        self.peers = {}

    def moved(self, dim, by=1, core=0):
        by %= len(self.at[dim])
        if (dim, by, core) not in self.peers:
            x, y, z, c = (steps[by if d == dim else core if d == CORE else 0] for d, steps in enumerate(self.at))
            self.peers[dim, by, core] = {"dp": ((x * RING + y) * RING + z) * PAIR + c}
        return self.peers[dim, by, core]


def meet(peers):
    barrier = pltpu.get_barrier_semaphore()
    for peer in peers:
        pl.semaphore_signal(barrier, inc=1, device_id=peer)
    pl.semaphore_wait(barrier, len(peers))


def remote(src, dst, send, recv, peer):
    return pltpu.make_async_remote_copy(src, dst, send, recv, device_id=peer)


def up(v):
    return v.astype(F32)


def call(kernel, outs, ins, scratch, name, vmem_limit=MOST, ident=None, out_specs=None, **more):
    return pl.pallas_call(
        kernel,
        out_shape=outs,
        in_specs=ins,
        out_specs=out_specs or [HBM] * len(outs),
        scratch_shapes=scratch,
        compiler_params=pltpu.CompilerParams(collective_id=ident, has_side_effects=ident is not None, vmem_limit_bytes=vmem_limit),
        name=name,
        **more,
    )


def odd(i):
    return lax.rem(i, 2)


def tiled(n, body, hooks=(), base=0):
    def one(i, _):
        body(i)
        for k, hook in hooks:
            pl.when(base + i == k)(hook)
        return _

    lax.fori_loop(0, n, one, 0)


class Loaded:
    def __init__(self, n, src, buf, sem):
        self.n, self.src, self.buf, self.sem = n, src, buf, sem

    def copy(self, i):
        slot = odd(i)
        return pltpu.make_async_copy(self.src(i), self.buf.at[slot], self.sem.at[slot])

    def start(self):
        self.copy(jnp.int32(0)).start()

    def ready(self, i):
        pl.when(i + 1 < self.n)(lambda: self.copy(i + 1).start())
        self.copy(i).wait()

    def take(self, i):
        self.ready(i)
        return odd(i)


def mm(a, b, across=0):
    return lax.dot_general(a, b, (((1,), (across,)), ((), ())), preferred_element_type=F32)


def tn(a, b):
    return lax.dot_general(a, b, (((0,), (0,)), ((), ())), preferred_element_type=F32).astype(BF)


def at(i, n, base=0):
    return pl.ds(pl.multiple_of(base + i * n, 128), n)


def fetch(pairs, sem):
    copies = [pltpu.make_async_copy(src, dst, sem.at[i]) for i, (src, dst) in enumerate(pairs)]
    for cp in copies:
        cp.start()
    return copies


class Cut:
    def __init__(self, gate):
        self.gate = gate
        self.width = HG // 2 if gate else HD
        self.n, self.rows = (1, ZROWS) if gate else (RING, DROWS)

    def dims(self, s):
        return (s, 1 - s, Z) if self.gate else (Z, s, 1 - s)

    def part(self, s, h, base=0):
        first = 384 if self.gate or s == 0 else 256
        return pl.ds(base + first, self.width - first) if h else pl.ds(base, first)

    def index(self, here, s, dim, r, done, cols):
        at = [here.at[d][r % RING] if d == dim else ALL if d in done else here.at[d][0] for d in (X, Y, Z)]
        return (at[X], at[Y]) + ((ALL,) if self.gate else (at[Z], s)) + (ALL, cols)


GATE, DOWN = Cut(True), Cut(False)


def ahead(k):
    return 1 if k in (0, 3, 4) else -1


SUM, OWN, GOT = range(3)
TILES = 6
TILE = FF // TILES
DOWN_SCRATCH = [vmem((TILES, TILE, HD), BF)] + [dma((TILES,))] * 2 + [dma((GOT + 1, TILES))]
HIDDEN = [vmem((2, T, TILE), BF), PAIR_SEM, vmem((TILES, PAIR, TILE, HD), BF)]
BLOCKS = (RING, RING, 1, ZROWS)
GATE_SCRATCH = [vmem((2, 2) + BLOCKS + (GATE.width,), BF)] * 3 + [PAIRS_SEM] * 2
GATE_SUMS, DOWN_SUMS = out((GOT + 1, 2) + BLOCKS + (HG,), BF), out((GOT + 1, FF, HD), BF)


class DownProduct:
    def __init__(self, here, hid, hbuf, hsem, halves, got, send, recv, outsem):
        self.here, self.halves, self.got, self.send, self.recv, self.outsem = here, halves, got, send, recv, outsem
        self.hidden = Loaded(TILES, lambda i: hid.at[:, at(i, TILE)], hbuf, hsem)
        self.hidden.start()

    def swap(self, i):
        _, theirs = self.here.at[CORE]
        return remote(self.halves.at[i, theirs], self.got.at[i], self.send.at[i], self.recv.at[i], self.here.moved(CORE))

    def put(self, od, i):
        mine, theirs = self.here.at[CORE]
        srcs = self.halves.at[i, theirs], self.halves.at[i, mine], self.got.at[i]
        return [pltpu.make_async_copy(src, od.at[k, at(i, TILE), :], self.outsem.at[k, i]) for k, src in enumerate(srcs)]

    def run(self, dy, od, hooks=()):
        mine, theirs = self.here.at[CORE]

        def add(i):
            self.swap(i).wait()
            self.halves[i, theirs] = (up(self.got[i]) + up(self.halves[i, mine])).astype(BF)
            for cp in self.put(od, i):
                cp.start()

        def body(i):
            full = tn(self.hidden.buf[self.hidden.take(i)], dy[...])
            for half in BOTH:
                self.halves[i, half] = full[:, half * HD : (half + 1) * HD]
            self.swap(i).start()
            pl.when(i > 0)(lambda: add(i - 1))

        tiled(TILES, body, hooks)
        add(TILES - 1)
        for i in range(TILES):
            for cp in self.put(od, i):
                cp.wait()


class GateProducts:
    def __init__(self, here, d, buf, sem, total, own, got, send, recv):
        self.here, self.sems = here, (send, recv)
        self.terms = total, own, got

        def src(i):
            t, (mine, theirs) = lax.rem(i, 4), here.at[CORE]
            return d.at[lax.div(i, 4), :, at(odd(i), GATE.width, jnp.where(t < 2, theirs, mine) * HG)]

        self.tiles = Loaded(8, src, buf, sem)
        self.tiles.start()

    def swap(self, w, t):
        send, recv = self.sems
        return remote(self.terms[SUM].at[w, t], self.terms[GOT].at[w, t], send.at[w, t], recv.at[w, t], self.here.moved(CORE))

    def put(self, og, sem, w, t):
        return [pltpu.make_async_copy(v.at[w, t], og.at[k, w, :, :, :, :, at(t, GATE.width)], sem.at[k, w, t]) for k, v in enumerate(self.terms)]

    def run(self, a, hooks=(), after=lambda w, t: None):
        total, own, got = self.terms

        def product(i):
            return tn(a[...], self.tiles.buf[self.tiles.take(i)]).reshape(BLOCKS + (GATE.width,))

        def matrix(w, _):
            def theirs(t):
                total[w, t] = product(4 * w + t)
                self.swap(w, t).start()

            def mine(t):
                own[w, t] = product(4 * w + 2 + t)
                self.swap(w, t).wait()
                total[w, t] = (up(got[w, t]) + up(own[w, t])).astype(BF)
                after(w, t)

            tiled(2, theirs, hooks, 4 * w)
            tiled(2, mine, hooks, 4 * w + 2)
            return _

        lax.fori_loop(0, 2, matrix, 0)


COLUMNS = [vmem((2, T, GATE.width), BF), PAIR_SEM]


PART = T // 4


def in_parts(body, at_once=T // PART):
    def some(i):
        for k in range(at_once):
            body(at(at_once * i + k, PART))

    tiled(T // (at_once * PART), some)


def normed(src, dst):
    def rows(i):
        r = at(i, PART)
        wide = up(src[r])
        dst[r] = (wide * lax.rsqrt(jnp.mean(wide**2, -1, keepdims=True) + 1e-6)).astype(BF)

    tiled(T // PART, rows)


def gated(gate, u):
    sig = jax.nn.sigmoid(gate)
    silu = gate * sig
    return (silu * u).astype(BF), u * (sig * (1 + gate * (1 - sig))), silu


class Stored:
    def __init__(self, dst, buf, sem):
        self.dst, self.buf, self.sem = dst, buf, sem

    def copy(self, i):
        slot = odd(i)
        return pltpu.make_async_copy(self.buf.at[slot], self.dst(i), self.sem.at[slot])

    def free(self, i):
        pl.when(i >= 2)(lambda: self.copy(i - 2).wait())

    def end(self, n):
        for i in (n - 2, n - 1):
            self.copy(jnp.int32(i)).wait()


HALVES = vmem((2, 2, D, WIDE), BF)
STATES = vmem((T, D), BF)


def forward_kernel(x, dy, wg, wu, wd, oa0, ohid0, ofg, ofu, oh1, ohid1, od1, og, od, vx, va, vhid, vdy, sem, osem, hsem, *refs):
    n, here = FF // WIDE, Place()
    meet([here.moved(CORE)])
    x_here, dy_here = fetch([(x, vx), (dy, vdy)], sem)
    wide = lambda ref, l: lambda i: ref.at[l, :, at(i, WIDE)]

    def put(i):
        return pltpu.make_async_copy(vhid.at[:, at(i, WIDE)], ohid0.at[:, at(i, WIDE)], hsem.at[i])

    def first(vw, wsem, vo, vsem):
        tiles = [Loaded(n, wide(w, 0), vw.at[k], wsem.at[k]) for k, w in enumerate((wg, wu))]
        outs = [Stored(lambda i, o=o: o.at[:, at(i, WIDE)], vo.at[k], vsem.at[k]) for k, o in enumerate((ofg, ofu))]
        for t in tiles:
            t.start()
        x_here.wait()
        normed(vx, va)
        a_out, = fetch([(va, oa0)], osem)

        def body(i):
            slot, _ = [t.take(i) for t in tiles]
            for o in outs:
                o.free(i)

            def rows(r):
                vhid[r, at(i, WIDE)], *factors = gated(*(mm(va[r], vw[k, slot]) for k in BOTH))
                for k in BOTH:
                    vo[k, slot, r] = factors[k]

            in_parts(rows)
            put(i).start()
            for o in outs:
                o.copy(i).start()

        tiled(n, body)
        for o in outs:
            o.end(n)
        a_out.wait()

    pl.run_scoped(first, HALVES, PAIRS_SEM, vmem((2, 2, T, WIDE), F32), PAIRS_SEM)

    def second(vw, wsem):
        tiles = Loaded(D // NT, lambda i: wd.at[0, :, at(i, NT)], vw, wsem)
        tiles.start()

        def body(i):
            slot, cols = tiles.take(i), at(i, NT)

            def rows(r):
                vx[r, cols] = (up(vx[r, cols]) + up(mm(vhid[r], vw[slot]).astype(BF))).astype(BF)

            in_parts(rows)

        tiled(D // NT, body)

    pl.run_scoped(second, vmem((2, FF, NT), BF), PAIR_SEM)
    for i in range(n):
        put(i).wait()

    def third(vw, wsem, vd, dsem, vo, vsem):
        tiles = [Loaded(n, wide(w, 1), vw.at[k], wsem.at[k]) for k, w in enumerate((wg, wu))]
        tiles.append(Loaded(n, lambda i: wd.at[1, at(i, WIDE), :], vd, dsem))
        outs = [Stored(lambda i, o=o: o.at[:, at(i, WIDE)], vo.at[k], vsem.at[k]) for k, o in enumerate((od1.at[0], od1.at[1], ohid1))]
        for t in tiles:
            t.start()
        normed(vx, va)
        kept = fetch([(vx, oh1)], osem)
        dy_here.wait()

        def body(i):
            slot, *_ = [t.take(i) for t in tiles]
            for o in outs:
                o.free(i)

            def rows(r):
                hid, *factors = gated(*(mm(va[r], vw[k, slot]) for k in BOTH))
                dhid = up(mm(vdy[r], vd[slot], 1).astype(BF))
                vo[2, slot, r] = hid
                for k in BOTH:
                    vo[k, slot, r] = (dhid * factors[k]).astype(BF)

            in_parts(rows)
            for o in outs:
                o.copy(i).start()

        tiled(n, body)
        for o in outs:
            o.end(n)
        for cp in kept:
            cp.wait()

    pl.run_scoped(third, HALVES, PAIRS_SEM, vmem((2, WIDE, D), BF), PAIR_SEM, vmem((3, 2, T, WIDE), BF), dma((3, 2)))

    def fourth(*local):
        k = len(HIDDEN)
        down = DownProduct(here, ohid1, *local[:k], *refs[: len(DOWN_SCRATCH)])
        *gate_refs, gsem = refs[len(DOWN_SCRATCH) :]
        gates = GateProducts(here, od1, *local[k:], *gate_refs)

        def put(w, t):
            for cp in gates.put(og, gsem, w, t):
                cp.start()

        down.run(vdy, od)
        gates.run(va, after=put)
        for w in BOTH:
            for t in BOTH:
                for cp in gates.put(og, gsem, w, t):
                    cp.wait()

    pl.run_scoped(fourth, *HIDDEN, *COLUMNS, *GATE_SCRATCH[:GOT])


def forward(x, dy, wg, wu, wd):
    states, hidden = out((T, D), BF), out((T, FF), BF)
    outs = [states, hidden, out((T, FF), F32), out((T, FF), F32), states, hidden, out((2, T, FF), BF), GATE_SUMS, DOWN_SUMS]
    scratch = [STATES] * 2 + [vmem((T, FF), BF), STATES, PAIR_SEM, PAIR_SEM, dma((FF // WIDE,))]
    scratch += DOWN_SCRATCH + GATE_SCRATCH[GOT:] + [dma((GOT + 1, 2, 2))]
    a0, hid0, by_gate, by_up, h1, _, d1, pg, pd = call(forward_kernel, outs, [HBM] * 5, scratch, "forward", ident=1)(x, dy, wg, wu, wd)
    return a0, hid0, by_gate, by_up, h1, d1, pg, pd


PHASES, COPIES = 3, 6
NAMES = ("r1", "o1", "k2", "r2", "t3", "k3", "r3", "send", "recv", "own")


class Summed:
    def __init__(self, here, cut, src, b, u, s):
        self.here, self.cut, self.src, self.us, self.s, self.dims = here, cut, src, (u, s), s, cut.dims(s)
        self.got, self.kept = [b[k] for k in ("r1", "r2", "r3")], [b[k] for k in ("o1", "k2", "k3")]
        self.t3, self.sems, self.direct = b["t3"], (b["send"], b["recv"], b["own"]), isinstance(src, tuple)

    def block(self, phase, r, cols=ALL, first=()):
        dim = self.dims[phase]
        i = self.here.at[dim][r % RING]
        if phase == 2:
            return self.us + first + (i, ALL, cols)
        second = phase == 1 and not self.cut.gate and self.s
        return self.us + first + ((ALL, i) if second else (i, ALL)) + (ALL, cols)

    def first(self, kind, r, h):
        if self.direct:
            ref, lead, base = self.src[kind], self.us, 0
        else:
            ref, lead, base = self.src, (kind,) + (self.us[:1] if self.cut.gate else ()), self.s * self.cut.width if self.cut.gate else 0
        return ref.at[lead + self.cut.index(self.here, self.s, self.dims[0], r, self.dims, self.cut.part(self.s, h, base))]

    def term(self, n, cols=ALL, r=0):
        if self.direct:
            i = self.here.at[self.dims[0]][r % RING]
            at_, terms = [self.us + ((n, i) if self.s else (i, n)) + (ALL, ALL, cols)] * 2, self.src[OWN:]
        else:
            at_, terms = [self.us + (k, n, ALL, ALL, cols) for k in BOTH], [self.kept[0]] * 2
        return sum(up(ref[i]) for ref, i in zip(terms, at_))

    def at(self, phase, kind, cols=ALL):
        return self.us + (kind,) + (ALL,) * (PHASES - phase) + (cols,)

    def copy(self, phase, k):
        kind, h = k // 2, k % 2
        cols = self.cut.part(self.s, h)
        got = self.got[phase]
        r = (2, -ahead(h), 0)[kind]
        if kind == 2:
            src = got.at[self.at(phase, 0, cols)]
        elif phase == 0:
            src = self.first(SUM, r, h)
        elif phase == 1:
            src = self.got[0].at[self.block(1, r, cols, (2,))]
        else:
            src = self.t3.at[self.block(2, r, cols)]
        send, recv, _ = self.sems
        i = self.us + (phase * COPIES + k,)
        return remote(src, got.at[self.at(phase, kind, cols)], send.at[i], recv.at[i], self.here.moved(self.dims[phase], ahead(k)))

    def own(self, k):
        kind, h = k // 2, k % 2
        cols, copies = self.cut.part(self.s, h), []
        for term in () if self.direct else BOTH:
            dst = self.kept[0].at[self.us + (term,) + (ALL,) * PHASES + (cols,)]
            copies.append(pltpu.make_async_copy(self.first(OWN + term, 0 if kind else ahead(h), h), dst, self.sems[2].at[self.us + (k, term)]))
        return copies

    def start(self, part):
        for h in BOTH:
            self.copy(0, 2 * part + h).start()
            for cp in [] if part else self.own(h):
                cp.start()

    def arrive(self, ks):
        for k in ks:
            for cp in self.own(k):
                cp.wait()

    def pass_on(self, phase):
        got, kept = self.got[phase], self.kept[phase]
        for h in BOTH:
            self.copy(phase, h).wait_recv()
            cols = self.cut.part(self.s, h)
            if phase:
                i = self.at(phase, 0, cols)
                got[i] = (up(got[i]) + kept[self.block(phase, ahead(h), cols)]).astype(BF)
            else:
                self.arrive([h])

                def add(n):
                    i = self.us + (0, n, ALL, ALL, cols)
                    got[i] = (up(got[i]) + self.term(n, cols, ahead(h))).astype(BF)

                tiled(RING, add)
            self.copy(phase, 4 + h).start()
        for h in () if phase else BOTH:
            for cp in self.own(2 + h):
                cp.start()

    def finish(self, phase):
        for k in range(2, COPIES):
            self.copy(phase, k).wait_recv()
        got, kept = self.got[phase], self.kept[phase]
        if phase:
            return kept[self.block(phase, 0)] + up(got[self.us + (2,)]) + up(got[self.us + (1,)])
        self.arrive((2, 3))

        def add(n):
            total = self.term(n) + up(got[self.us + (2, n)]) + up(got[self.us + (1, n)])
            self.kept[1][self.us + (n,)] = total
            got[self.us + (2, n)] = total.astype(BF)

        tiled(RING, add)

    def starts(self, phase):
        for k in range(4):
            self.copy(phase, k).start()


class Sums:
    def __init__(self, here, og, od, refs):
        self.here = here
        n = len(NAMES)
        bufs = [dict(zip(NAMES, refs[i : i + n])) for i in (0, n)]
        self.f3, self.f4, self.ce, self.cr, self.co, self.fd, self.dr, self.csend, self.crecv, self.putsem = refs[2 * n :]
        self.gate, self.upper = ([Summed(here, GATE, og, bufs[0], u, s) for s in BOTH] for u in BOTH)
        self.down = [Summed(here, DOWN, od, bufs[1], 0, s) for s in BOTH]
        self.puts = []
        self.f3[ZROWS : ZROWS + 8] = jnp.zeros((8, GATE.width), F32)
        self.f4[PAD : PAD + 8] = jnp.zeros((8, HG), F32)

    def begin(self, streams):
        for part in BOTH:
            for st in streams:
                st.start(part)

    def second(self, st):
        total = st.finish(1)
        if st.cut.gate:
            self.f3[0:ZROWS] = total[0]
            for i in range(RING):
                rows = self.f3[i * PAIR * ROWS : i * PAIR * ROWS + PAD]
                st.kept[2][st.us + (i,)] = rows
                st.t3[st.us + (i,)] = rows.astype(BF)
        else:
            st.kept[2][st.us] = total
            st.t3[st.us] = total.astype(BF)

    def step(self, n, *streams):
        for st in streams:
            if n % 2 == 0:
                st.pass_on(n // 2)
            else:
                if n == 1:
                    st.finish(0)
                else:
                    self.second(st)
                st.starts(n // 2 + 1)

    def swap(self, u):
        src, dst = (self.fd.at[self.here.at[CORE][1]], self.dr) if u == 2 else (self.ce.at[u], self.cr.at[u])
        return remote(src, dst, self.csend.at[u], self.crecv.at[u], self.here.moved(CORE))

    def last(self, u):
        if u == 2:
            for st in self.down:
                self.fd[st.s] = st.finish(2).astype(BF)
            parts = [up(self.fd[s]) for s in BOTH]
        else:
            for st in self.upper if u else self.gate:
                self.f4[0:PAD, st.s * GATE.width : (st.s + 1) * GATE.width] = st.finish(2)
            low, high = self.f4[0:16], self.f4[ROWS : ROWS + 16]
            first = self.here.at[CORE][0] == 0
            self.co[u] = jnp.where(first, low, high).astype(BF)
            self.ce[u] = jnp.where(first, high, low).astype(BF)
            valid = lax.broadcasted_iota(jnp.int32, (PAD, HG), 0) < PAIR * ROWS
            parts = [jnp.where(valid, up(self.f4[0:PAD].astype(BF)), 0.0)]
        self.swap(u).start()
        return sum(squares(v) for v in parts)

    def put(self, src, dst):
        self.puts.append(pltpu.make_async_copy(src, dst, self.putsem.at[len(self.puts)]))
        self.puts[-1].start()

    def results(self, gg, gd):
        mine, theirs = self.here.at[CORE]
        for u in range(3):
            n, dst = (HD, gd) if u == 2 else (HG, gg.at[u])
            self.put(self.fd.at[mine] if u == 2 else self.co.at[u], dst.at[:, at(mine, n)])
            self.swap(u).wait()
            self.put(self.dr if u == 2 else self.cr.at[u], dst.at[:, at(theirs, n)])

    def drain(self):
        for st in self.down + self.gate + self.upper:
            for k in range(PHASES * COPIES):
                st.copy(k // COPIES, k % COPIES).wait_send()
        for cp in self.puts:
            cp.wait()


def squares(v):
    v = v * v
    rows = sum(v[i : i + 8] for i in range(0, v.shape[0], 8))
    return sum(rows[:, i : i + 128] for i in range(0, v.shape[1], 128))


LANES = vmem((8, 128), F32)


def sums_scratch(direct):
    scratch = []
    for cut, units in ((GATE, 2), (DOWN, 1)):
        us, block, width = (units, 2), (cut.n, cut.rows, cut.width), cut.width
        terms = LANES if direct and cut.gate else vmem(us + (2, RING) + block, BF)
        scratch += [vmem(us + (3, RING) + block, BF), terms, vmem(us + (RING,) + block, F32), vmem(us + (3,) + block, BF)]
        scratch += [vmem(us + (RING, PAD, width), t) for t in (BF, F32)] + [vmem(us + (3, PAD, width), BF)]
        scratch += [dma(us + (PHASES * COPIES,))] * 2 + [dma(us + (4, 2))]
    scratch += [vmem((ZROWS + 8, GATE.width), F32), vmem((PAD + 8, HG), F32)] + [vmem((2, 16, HG), BF)] * 3
    return scratch + [vmem((2, DROWS, HD), BF), vmem((DROWS, HD), BF)] + [dma((3,))] * 2 + [dma((7,))]


ROWS_OUT = [out((2, 16, FF), BF), out((DROWS, D), BF), out((8, 128), F32)]
DOWN_BLOCKS = (GOT + 1, RING, RING, RING, PAIR, DROWS, HD)


def stages(here):
    along = lambda d, core=0: [here.moved(d, r, core) for r in range(1, RING)]
    return [here.moved(CORE)] + along(Z) + along(Z, 1), along(Y), along(X)


def all_peers(here):
    return sum(stages(here), [])


def over_all(here, total, nb, nr, send, recv):
    n = 0
    for stage, peers in enumerate(stages(here)):
        nb[stage] = total
        copies = []
        for peer in peers:
            copies.append(remote(nb.at[stage], nr.at[n], send.at[n], recv.at[n], peer))
            copies[-1].start()
            n += 1
        for i, cp in enumerate(copies):
            cp.wait()
            total = total + nr[n - len(copies) + i]
    return total


def back_kernel(d, h1, dy, wg, wu, wd, by_gate, by_up, hid, pg, pd, od0, opd, gg, gd, osq, dx, vh, vy, nb, sem, state_sem, *refs):
    here = Place()
    n = len(DOWN_SCRATCH)
    sums = Sums(here, pg, pd, refs[n:])
    meet(all_peers(here))
    step = lambda n, streams: lambda: sums.step(n, *streams)
    early, late = zip(sums.down, sums.gate[:1] + sums.upper[:1], sums.gate[1:] + sums.upper[1:])
    sums.begin(early + late)
    states_here = fetch([(h1, vh), (dy, vy)], state_sem)

    def states(vd, vw, wsem):
        n = D // NT
        tiles = [Loaded(n, lambda i, w=w: w.at[1, at(i, NT), :], vw.at[k], wsem.at[k]) for k, w in enumerate((wg, wu))]
        loads = []
        for k in BOTH:
            loads += fetch([(d.at[k], vd.at[k])], sem.at[pl.ds(k, 1)])
            tiles[k].start()

        def body(i):
            k, i = lax.div(i, n), lax.rem(i, n)
            for which in BOTH:
                pl.when(k == which)(lambda: tiles[which].ready(i))
            before = jnp.where(k == 0, 0.0, up(dx[:, at(i, NT)]))
            dx[:, at(i, NT)] = (before + up(mm(vd[k], vw[k, odd(i)], 1).astype(BF))).astype(BF)

        hooks = [(n - 1, loads[1].wait), (n // 2, step(0, early)), (n + 1, step(0, late))]
        loads[0].wait()
        tiled(2 * n, body, hooks)

    pl.run_scoped(states, vmem((2, T, FF), BF), vmem((2, 2, NT, FF), BF), PAIRS_SEM)

    def norm_back(i):
        r = at(i, NT)
        wide, da = up(vh[r]), up(dx[r])
        scale = lax.rsqrt(jnp.mean(wide**2, -1, keepdims=True) + 1e-6)
        mean = jnp.mean(da * wide, -1, keepdims=True)
        dx[r] = (up(vy[r]) + up((da * scale - wide * (scale * scale * scale * mean)).astype(BF))).astype(BF)

    for cp in states_here:
        cp.wait()
    tiled(T // NT, norm_back)

    def hidden_back(vw, wsem, vf, fsem, vo, outsem):
        n = FF // WIDE
        tiles = [Loaded(n, lambda i: wd.at[0, at(i, WIDE), :], vw, wsem)]
        tiles += [Loaded(n, lambda i, f=f: f.at[:, at(i, WIDE)], vf.at[k], fsem.at[k]) for k, f in enumerate((by_gate, by_up))]
        outs = [Stored(lambda i, k=k: od0.at[k, :, at(i, WIDE)], vo.at[k], outsem.at[k]) for k in BOTH]
        for t in tiles:
            t.start()

        def body(i):
            slot, *_ = [t.take(i) for t in tiles]
            for o in outs:
                o.free(i)

            def rows(r):
                dhid = up(mm(dx[r], vw[slot], 1).astype(BF))
                for k in BOTH:
                    vo[k, slot, r] = (dhid * vf[k, slot, r]).astype(BF)

            in_parts(rows, 2)
            for o in outs:
                o.copy(i).start()

        tiled(n, body, [(1, step(1, early)), (3, step(1, late)), (4, step(2, early)), (5, step(2, late))])
        for o in outs:
            o.end(n)

    pl.run_scoped(hidden_back, vmem((2, WIDE, D), BF), PAIR_SEM, vmem((2, 2, T, WIDE), F32), PAIRS_SEM, vmem((2, 2, T, WIDE), BF), PAIRS_SEM)

    def last(*tile_refs):
        steps = [step(n, streams) for n in (3, 4) for streams in (early, late)]
        DownProduct(here, hid, *tile_refs, *refs[:n]).run(dx, opd, list(enumerate(steps)))

    pl.run_scoped(last, *HIDDEN)
    nb[...] = sum(sums.last(u) for u in (2, 0, 1))
    sums.results(gg, gd)
    sums.put(nb, osq)
    sums.drain()


def back(*args):
    *ins, pg, pd = args
    outs = [out((2, T, FF), BF), DOWN_SUMS] + ROWS_OUT
    scratch = [STATES] * 3 + [LANES, PAIR_SEM, PAIR_SEM] + DOWN_SCRATCH + sums_scratch(False)
    return call(back_kernel, outs, [HBM] * len(args), scratch, "back", ident=2)(*ins, pg, pd.reshape(DOWN_BLOCKS))


def end_kernel(a, d, pd, sq, gg, gd, osq, va, vsq, nb, nr, nsend, nrecv, sem, *refs):
    here = Place()
    n = len(COLUMNS + GATE_SCRATCH)
    gates = GateProducts(here, d, *refs[:n])
    sums = Sums(here, gates.terms, pd, refs[n:])
    a_here, sq_here = fetch([(a, va), (sq, vsq)], sem)
    meet(all_peers(here))
    sums.begin(sums.down)
    a_here.wait()
    (d0, d1), (g0, g1), (u0, u1) = sums.down, sums.gate, sums.upper

    def begin(new, *old):
        sums.begin([new])
        sums.step(0, *old)

    hooks = {2: lambda: begin(g0), 3: lambda: begin(g1, d0), 4: lambda: sums.step(0, d1), 5: lambda: sums.step(0, g0), 6: lambda: begin(u0, g1)}
    gates.run(va, hooks.items())
    sums.begin([u1])
    sums.step(1, g0, d0, g1)
    sums.step(0, u0)
    sums.step(1, d1)
    sums.step(0, u1)
    for n in (2, 3):
        sums.step(n, g0, d0, g1, d1)
    sums.step(1, u0, u1)
    sums.step(4, g0, d0, g1, d1)
    sums.step(2, u0, u1)
    total = sums.last(2) + sums.last(0)
    for n in (3, 4):
        sums.step(n, u0, u1)
    total += sums.last(1)
    sq_here.wait()
    nb[4] = over_all(here, total + vsq[...], nb, nr, nsend, nrecv)
    sums.put(nb.at[4], osq)
    sums.results(gg, gd)
    sums.drain()


def end(a, d, pd, sq):
    scratch = [STATES, LANES, vmem((5, 8, 128), F32), vmem((13, 8, 128), F32)] + [dma((13,))] * 2 + [PAIR_SEM]
    scratch += COLUMNS + GATE_SCRATCH + sums_scratch(True)
    return call(end_kernel, ROWS_OUT, [HBM] * 4, scratch, "end", ident=4)(a, d, pd.reshape(DOWN_BLOCKS), sq)


COUNT = 3 * L * D * FF


def adamw_kernel(gg0, gg1, gd0, gd1, norm, *refs):
    old, (wg, wu, wd), new, (ng, nd, win, wind, sg, sw, sem) = refs[:6], refs[6:9], refs[9:15], refs[15:]
    i = lax.axis_index("dp")
    start, off = pl.multiple_of(i * ROWS // 8 * 8, 8), i * ROWS % 8
    copies = [pltpu.make_async_copy((wg, wu)[u // L].at[u % L, pl.ds(start, 16), :], win.at[u], sem.at[u]) for u in range(PAIR * L)]
    copies.append(pltpu.make_async_copy(wd.at[:, pl.ds(pl.multiple_of(i * DROWS, 8), DROWS), :], wind, sem.at[PAIR * L]))
    for cp in copies:
        cp.start()
    factor = jnp.minimum(1.0, 0.5 * lax.rsqrt(jnp.full((1, 1), jnp.sum(norm[...])) / COUNT + 1e-30))
    for cp in copies:
        cp.wait()

    def step(k, w, g):
        g = g * factor
        m = 0.9 * old[k][...] + 0.1 * g
        v = 0.95 * old[k + 3][...] + 0.05 * g * g
        new[k][...], new[k + 3][...] = m, v
        return w - 0.02 * (m * lax.rsqrt(v + 1e-8) + 0.1 * w)

    for k in BOTH:
        for l in BOTH:
            w = up(win[k * L + l])
            rows = w[0:ROWS]
            for skip in (2, 4, 6):
                rows = jnp.where(off == skip, w[skip : skip + ROWS], rows)
            sw[:, l, :] = rows
            sg[:, l, :] = up((gg0, gg1)[l][k])[0:ROWS]
        sw[...] = step(k, sw[...], sg[...])
        for l in BOTH:
            ng[k * L + l, 0:ROWS] = sw[:, l, :].astype(BF)
    nd[...] = step(2, up(wind[...]), jnp.stack([up(gd0[...]), up(gd1[...])])).astype(BF)


def adamw(sums, norm, moments, weights):
    weights = [pltpu.with_memory_space_constraint(w, pltpu.HBM) for w in weights]
    flip = lambda k, t: t if k % 3 == 2 else jnp.swapaxes(t, 0, 1)
    moments = [flip(k, t) for k, t in enumerate(moments)]
    outs = [out(t.shape, F32) for t in moments] + [out((PAIR * L, 16, FF), BF), vmem((L, DROWS, D), BF)]
    scratch = [vmem((PAIR * L, 16, FF), BF), vmem((L, DROWS, D), BF)] + [vmem((ROWS, L, FF), F32)] * 2 + [dma((PAIR * L + 1,))]
    *new, ng, nd = call(adamw_kernel, outs, [VM] * 11 + [HBM] * 3, scratch, "adamw", MOST - 5 * 2**17, out_specs=[VM] * 8)(*sums, norm, *moments, *weights)
    return [flip(k, t) for k, t in enumerate(new)], ng, nd


class Gathered:
    def __init__(self, here, cut, refs, b, u, s):
        self.here, self.cut, self.refs, self.b, self.u, self.s = here, cut, refs, b, u, s
        self.order = cut.dims(s)[::-1]
        n, first = (HG, s * cut.width) if cut.gate else (HD, 0)
        self.whole = [pl.ds(pl.multiple_of(c * n + first, 128), cut.width) for c in here.at[CORE]]

    def ref(self, at):
        return self.refs[self.u // L].at[(self.u % L,) + at]

    def copy(self, phase, k):
        dim, back = self.order[phase], k % 2
        cols = self.whole[0]
        if k >= 2:
            cols = self.cut.part(self.s, back, cols.start)
        v = self.ref(self.cut.index(self.here, self.s, dim, 0 if k < 2 else 2 * back - 1, self.order[:phase], cols))
        i = phase * 4 + k
        return remote(v, v, self.b[0].at[self.u, self.s, i], self.b[1].at[self.u, self.s, i], self.here.moved(dim, 1 - 2 * back))

    def across(self, r, core=0):
        v = self.ref(self.cut.index(self.here, self.s, self.order[2], r, self.order, self.whole[core]))
        i = PHASES * 4 + r % RING
        return remote(v, v, self.b[0].at[self.u, self.s, i], self.b[1].at[self.u, self.s, i], self.here.moved(CORE))

    def start(self, phase):
        for k in BOTH:
            self.copy(phase, k).start()
        if phase == 2:
            self.across(0).start()

    def forward(self, phase):
        for k in BOTH:
            self.copy(phase, k).wait_recv()
            self.copy(phase, 2 + k).start()
            if phase == 2:
                self.across(2 * k - 1).start()

    def end(self, phase):
        for k in BOTH:
            self.copy(phase, 2 + k).wait_recv()
        if phase < 2:
            self.start(phase + 1)
        else:
            self.across(2).start()


def ag_kernel(wg, wd, o0, o1, od, cs, cx, zb, zf, zm, csend, crecv, zsend, zrecv, gsend, grecv, dsend, drecv):
    here = Place()
    (x, y, z, c), other = (steps[0] for steps in here.at), here.moved(CORE)
    meet([here.moved(d, r) for d in (X, Y, Z) for r in (1, -1)] + [other])
    half = lambda which, n: pl.ds(pl.multiple_of(which * n, 128), n)
    mine, theirs = c, 1 - c

    def swap_g(u):
        return remote(wg.at[u, :, half(theirs, HG)], cx.at[u], csend.at[u], crecv.at[u], other)

    def swap_d(l, core, which):
        there = od.at[l, x, y, z, core, :, half(which, HD)]
        return remote(wd.at[l, :, half(theirs, HD)], there, csend.at[PAIR * L + l], crecv.at[PAIR * L + l], other)

    for u in range(PAIR * L):
        swap_g(u).start()
    for l in BOTH:
        swap_d(l, c, theirs).start()
        od[l, x, y, z, c, :, half(mine, HD)] = wd[l, :, half(mine, HD)]

    def zcopy(s, k):
        back = k % 2
        cols = GATE.part(s, back, s * GATE.width) if k >= 2 else pl.ds(s * GATE.width, GATE.width)
        v = zb.at[here.at[Z][0 if k < 2 else (2 * back - 1) % RING], :, cols]
        return remote(v, v, zsend.at[s, k], zrecv.at[s, k], here.moved(Z, 1 - 2 * back))

    for u in range(PAIR * L):
        swap_g(u).wait_recv()
        own, got = up(wg[u, :, half(mine, HG)]), up(cx[u])
        for core in range(PAIR):
            row = (u * PAIR + core) * ROWS
            cs[row : row + ROWS] = jnp.where(c == core, own, got)[0:ROWS]
    for s in BOTH:
        cols = slice(s * GATE.width, (s + 1) * GATE.width)
        zb[z, :, cols] = cs[:, cols].astype(BF)
        for k in BOTH:
            zcopy(s, k).start()
    gate = [Gathered(here, GATE, (o0, o1), (gsend, grecv), u, s) for u in range(PAIR * L) for s in BOTH]
    down = [Gathered(here, DOWN, (od,), (dsend, drecv), l, s) for l in BOTH for s in BOTH]
    for l in BOTH:
        swap_d(l, 1 - c, mine).wait_recv()
    for st in down:
        st.start(0)
    for s in BOTH:
        for k in BOTH:
            zcopy(s, k).wait_recv()
            zcopy(s, 2 + k).start()
    for st in down:
        st.forward(0)
    for st in down:
        st.end(0)

    for s in BOTH:
        cols = slice(s * GATE.width, (s + 1) * GATE.width)
        for k in range(2, 4):
            zcopy(s, k).wait_recv()
        for i in range(RING):
            zm[...] = up(zb[i, :, cols])
            for u in range(PAIR * L):
                n = PAIR * ROWS
                zf[u, i * n : i * n + n] = zm[u * n : u * n + n]
        for st in gate[s::2]:
            (o0, o1)[st.u // L][st.u % L, x, y, 0, :, st.whole[0]] = zf[st.u].astype(BF)
            st.start(1)
    both = gate[: L * 2] + down[:2] + gate[L * 2 :] + down[2:]
    for phase in (1, 2):
        for st in both:
            st.forward(phase)
        for st in both:
            st.end(phase)
    for u in range(PAIR * L):
        swap_g(u).wait_send()
    for l in BOTH:
        swap_d(l, c, theirs).wait_send()
    for s in BOTH:
        for k in range(4):
            zcopy(s, k).wait_send()
    for st in both:
        for phase in range(1 if st.cut.gate else 0, PHASES):
            for k in range(4):
                st.copy(phase, k).wait_send()
        for r in range(RING):
            st.across(r).wait_send()
            st.across(r, 1).wait_recv()


def ag(wg, wd):
    block = (RING, RING, 1, ZROWS, FF)
    outs = [pltpu.VMEM((L,) + block, BF)] * 2 + [pltpu.VMEM((L, RING, RING, RING, PAIR, DROWS, D), BF)]
    n, sems = PAIR * L, PHASES * 4 + RING
    scratch = [vmem((ZROWS, HG), F32), vmem((n, 16, HG), BF), vmem((RING, ZROWS, HG), BF), vmem((n, ZROWS, GATE.width), F32), vmem((ZROWS, GATE.width), F32)]
    scratch += [dma((n + L,))] * 2 + [dma((2, 4))] * 2 + [dma((n, 2, sems))] * 2 + [dma((L, 2, sems))] * 2
    return call(ag_kernel, outs, [VM] * 2, scratch, "ag", vmem_limit=3 * 2**20, ident=3, out_specs=[VM] * 3)(wg, wd)


def put_kernel(*refs):
    *refs, sem = refs
    n = len(refs) // 2
    pairs = [(refs[k].at[l, x], refs[n + k].at[l, x]) for k in range(n) for l in BOTH for x in range(RING)]
    for cp in fetch(pairs, sem):
        cp.wait()


def put(weights):
    n = len(weights)
    return call(put_kernel, [out(w.shape, BF) for w in weights], [VM] * n, [dma((n * L * RING,))], "put", vmem_limit=2**20)(*weights)


def device_step(x, dy, wg, wu, wd, *moments):
    x, dy = x[0], dy[0]
    a0, hid0, by_gate, by_up, h1, d1, pg1, pd1 = forward(x, dy, wg, wu, wd)
    d0, pd0, gg1, gd1, squares1 = back(d1, h1, dy, wg, wu, wd, by_gate, by_up, hid0, pg1, pd1)
    gg0, gd0, norm = end(a0, d0, pd0, squares1)
    moments, ng, nd = adamw((gg0, gg1, gd0, gd1), norm, moments, (wg, wu, wd))
    return (*(new.reshape(w.shape) for new, w in zip(put(ag(ng, nd)), (wg, wu, wd))), *moments)


def solution(mesh):
    rows, moment, whole = P(("rep", "dp")), P(None, "dp"), P()
    return jax.shard_map(
        device_step,
        mesh=mesh,
        in_specs=(rows,) * 2 + (whole,) * 3 + (moment,) * 6,
        out_specs=(P("rep"),) * 3 + (P("rep", "dp"),) * 6,
        check_vma=False,
    )
```
